32 devices in a mesh: gx: 4 (over y, x), gy: 8 (over z, core).
Axes of the slice: x: 2, y: 2, z: 4, core: 2. Of those that a mesh axis runs over, the one named last changes fastest.
Arguments:
- features: bfloat16 [32, 32, 64, 128], P(None, 'gx', 'gy'), may hold values from -6 to 6
- weight_two: bfloat16 [27, 32, 32], replicated, may hold values from -0.21875 to 0.21875
- bias_two: float32 [32], replicated, may hold values from -3 to 3
- weight_three: bfloat16 [27, 64, 32], replicated, may hold values from -0.21875 to 0.21875
- bias_three: float32 [64], replicated, may hold values from -3 to 3
- weight_four: bfloat16 [27, 128, 64], replicated, may hold values from -0.25 to 0.25
- bias_four: float32 [128], replicated, may hold values from -3 to 3
Outputs:
- level_two: bfloat16 [32, 32, 64, 128], P(None, 'gx', 'gy')
- level_three: bfloat16 [64, 16, 32, 64], P(None, 'gx', 'gy')
- bottleneck: bfloat16 [128, 8, 16, 32], P(None, None, None, 'gy')
The draws below stay inside these ranges and needn't reach their ends.
All inputs are finite; a program needn't handle non-finite values.
Results may differ from the reference program's by a relative error of at most 0.0085.
Values may be sent and summed in bfloat16 or wider, within the bound.
No kernel may reach another device: no remote copies, remote signals or barrier semaphores. Data moves between devices by JAX's collectives and lax.ppermute only.
A program may use at most 64 MiB of HBM per device.

```python
import jax
import jax.numpy as jnp
from jax import lax

C2 = 32
C3 = 64
C4 = 128
NZ = 128
NX = 32
NY = 64


def steps_of(stream_key, dims, pieces, smallest, top_value):
    loudness = 1.0
    for dim, shards_of in pieces:
        heights = jax.random.uniform(jax.random.fold_in(jax.random.fold_in(stream_key, 6), dim), (shards_of,), jnp.float32, smallest / len(pieces), top_value / len(pieces))
        loudness = loudness * jnp.repeat(jnp.exp(heights), dims[dim] // shards_of).reshape((-1,) + (1,) * (len(dims) - 1 - dim))
    return loudness


def scatter_about(stream_key, shape, width, bound, cuts=(), dtype=jnp.bfloat16):
    gain = steps_of(stream_key, shape, cuts, -0.22, 0.18) if cuts else 1.0
    drawn = jax.random.normal(stream_key, shape, jnp.float32) * width * gain
    return jnp.minimum(jnp.maximum(drawn, -bound), bound).astype(dtype)


def setup_inputs(seed: int = 0) -> dict:
    splits = jax.random.split(jax.random.key(seed), 8)
    features = scatter_about(splits[0], (C2, NX, NY, NZ), 1.0, 6.0, ((1, 4), (2, 8)))
    weight_two = scatter_about(splits[1], (27, C2, C2), (27 * C2) ** -0.5, 0.21875)
    bias_two = scatter_about(splits[2], (C2,), 0.5, 3.0, (), jnp.float32)
    weight_three = scatter_about(splits[3], (27, C3, C2), (27 * C2) ** -0.5, 0.21875)
    bias_three = scatter_about(splits[4], (C3,), 0.5, 3.0, (), jnp.float32)
    weight_four = scatter_about(splits[5], (27, C4, C3), (9 * C3) ** -0.5, 0.25)
    bias_four = scatter_about(splits[6], (C4,), 0.5, 3.0, (), jnp.float32)
    return dict(features=features, weight_two=weight_two, bias_two=bias_two, weight_three=weight_three, bias_three=bias_three, weight_four=weight_four, bias_four=bias_four)


def convolve(source, weights, bias_values):
    in_channels = source.shape[0]
    out_channels = weights.shape[1]
    padded = jnp.pad(source.astype(jnp.float32), ((0, 0), (1, 1), (1, 1), (1, 1)), mode="wrap")
    kernel = weights.astype(jnp.float32).reshape(3, 3, 3, out_channels, in_channels).transpose(3, 4, 0, 1, 2)
    result = lax.conv_general_dilated(padded[None], kernel, (1, 1, 1), "VALID", precision=lax.Precision.HIGHEST)
    result = result[0] + bias_values.astype(jnp.float32)[:, None, None, None]
    return jax.nn.leaky_relu(result, 0.1).astype(jnp.bfloat16)


def average_pool(source):
    channels, extent_x, extent_y, extent_z = source.shape
    blocks = source.astype(jnp.float32).reshape(channels, extent_x // 2, 2, extent_y // 2, 2, extent_z // 2, 2)
    return blocks.mean(axis=(2, 4, 6)).astype(jnp.bfloat16)


def reference(features, weight_two, bias_two, weight_three, bias_three, weight_four, bias_four):
    level_two = convolve(features, weight_two, bias_two)
    level_three = convolve(average_pool(level_two), weight_three, bias_three)
    bottleneck = convolve(average_pool(level_three), weight_four, bias_four)
    return level_two, level_three, bottleneck
```

```python
import functools

import jax
import jax.numpy as jnp
from jax import lax
from jax.experimental import pallas as pl
from jax.experimental.pallas import tpu as pltpu
from jax.sharding import PartitionSpec as P

VMEM = pl.BlockSpec(memory_space=pltpu.VMEM)


def leaky(t):
    return jnp.where(t >= 0, t, 0.1 * t)


def shift_exchange(low, high, axis):
    count = lax.axis_size(axis)
    below = lax.ppermute(high, axis, [(i, (i + 1) % count) for i in range(count)])
    above = lax.ppermute(low, axis, [((i + 1) % count, i) for i in range(count)])
    return below, above


def pair_exchange(low, high, axis):
    count = lax.axis_size(axis)
    if count % 2:
        return shift_exchange(low, high, axis)
    even = lax.axis_index(axis) % 2 == 0
    inner = [(i, i + 1 if i % 2 == 0 else i - 1) for i in range(count)]
    outer = [(i, (i - 1) % count if i % 2 == 0 else (i + 1) % count) for i in range(count)]
    from_outer = lax.ppermute(jnp.where(even, low, high), axis, outer)
    from_inner = lax.ppermute(jnp.where(even, high, low), axis, inner)
    below = jnp.where(even, from_outer, from_inner)
    above = jnp.where(even, from_inner, from_outer)
    return below, above


def level_two_kernel(cells, left, right, below, above, mix, bias, pool, out, pooled, rolled):
    extent_x, extent_y, channels, depth = cells.shape

    def fill(value, x, y):
        rolled[1, x, y] = value
        wide = value.astype(jnp.float32)
        rolled[0, x, y] = pltpu.roll(wide, 1, 1).astype(value.dtype)
        rolled[2, x, y] = pltpu.roll(wide, depth - 1, 1).astype(value.dtype)

    for y in range(extent_y):
        fill(left[y], 0, y + 1)
        fill(right[y], extent_x + 1, y + 1)
        for x in range(extent_x):
            fill(cells[x, y], x + 1, y + 1)
    for x in range(extent_x + 2):
        fill(below[x], x, 0)
        fill(above[x], x, extent_y + 1)
    offset = bias[...]
    for bx in range(0, extent_x, 2):
        for by in range(0, extent_y, 4):
            stacked = jnp.concatenate(
                [
                    rolled[:, bx : bx + 4, y : y + 4].reshape(48 * channels, depth)
                    for y in (by, by + 2)
                ],
                axis=1,
            )
            result = jnp.dot(mix[...], stacked, preferred_element_type=jnp.float32)
            result = leaky(result + offset).astype(jnp.bfloat16)
            for half in range(2):
                parts = []
                for dx in range(2):
                    for dy in range(2):
                        row = (2 * dx + dy) * channels
                        part = result[row : row + channels, half * depth : (half + 1) * depth]
                        out[bx + dx, by + 2 * half + dy] = part
                        parts.append(part)
                mean = jnp.dot(
                    jnp.concatenate(parts, axis=1), pool[...], preferred_element_type=jnp.float32
                )
                pooled[bx // 2, by // 2 + half] = mean.astype(jnp.bfloat16)


def level_two_conv(cells, left, right, below, above, weights, bias_values):
    extent_x, extent_y, channels, depth = cells.shape
    taps = weights.reshape(3, 3, 3, channels, channels)
    blocks = [
        jnp.pad(taps, ((dx, 1 - dx), (dy, 1 - dy), (0, 0), (0, 0), (0, 0)))
        .transpose(3, 2, 0, 1, 4)
        .reshape(channels, 48 * channels)
        for dx in range(2)
        for dy in range(2)
    ]
    mix = jnp.concatenate(blocks, axis=0)
    bias = jnp.tile(bias_values, 4)[:, None]
    source = lax.broadcasted_iota(jnp.int32, (4 * depth, depth), 0) % depth // 2
    target = lax.broadcasted_iota(jnp.int32, (4 * depth, depth), 1) % (depth // 2)
    pool = jnp.where(source == target, 0.125, 0.0).astype(jnp.bfloat16)
    return pl.pallas_call(
        level_two_kernel,
        name="conv_two",
        out_shape=(
            jax.ShapeDtypeStruct(cells.shape, jnp.bfloat16),
            jax.ShapeDtypeStruct((extent_x // 2, extent_y // 2, channels, depth), jnp.bfloat16),
        ),
        in_specs=[VMEM] * 8,
        out_specs=(VMEM, VMEM),
        scratch_shapes=[
            pltpu.VMEM((3, extent_x + 2, extent_y + 2, channels, depth), jnp.bfloat16)
        ],
    )(cells, left, right, below, above, mix, bias, pool)


def level_three_kernel(cells, left, right, below, above, mix, bias, pool, out, pooled, paired):
    extent_x, extent_y, channels, lanes = cells.shape
    depth = lanes // 2
    out_channels = mix.shape[1]

    def column(x, y):
        if y == 0:
            return below[x]
        if y == extent_y + 1:
            return above[x]
        if x == 0:
            return left[y - 1]
        if x == extent_x + 1:
            return right[y - 1]
        return cells[x - 1, y - 1]

    first = lax.broadcasted_iota(jnp.int32, (channels, lanes), 1) < depth
    for x in range(extent_x + 2):
        for y in range(extent_y + 1):
            both = jnp.where(
                first, column(x, y).astype(jnp.float32), column(x, y + 1).astype(jnp.float32)
            )
            place = lax.broadcasted_iota(jnp.int32, (channels, lanes), 1) % depth
            up = jnp.where(place == 0, pltpu.roll(both, lanes - depth + 1, 1), pltpu.roll(both, 1, 1))
            down = jnp.where(
                place == depth - 1, pltpu.roll(both, depth - 1, 1), pltpu.roll(both, lanes - 1, 1)
            )
            paired[x, y, 0] = up.astype(jnp.bfloat16)
            paired[x, y, 1] = both.astype(jnp.bfloat16)
            paired[x, y, 2] = down.astype(jnp.bfloat16)
    offset = bias[...]
    for py in range(extent_y // 2):
        for px in range(extent_x // 2):
            stacked = jnp.concatenate(
                [
                    jnp.concatenate(
                        [
                            paired[x + a, 2 * py + c].reshape(3 * channels, lanes)
                            for a in range(3)
                            for c in range(3)
                        ],
                        axis=0,
                    )
                    for x in (2 * px, 2 * px + 1)
                ],
                axis=1,
            )
            result = lax.dot_general(
                mix[...], stacked, (((0,), (0,)), ((), ())), preferred_element_type=jnp.float32
            )
            result = leaky(result + offset).astype(jnp.bfloat16)
            out[2 * px, py] = result[:, :lanes]
            out[2 * px + 1, py] = result[:, lanes:]
            mean = lax.dot_general(
                pool[...], result, (((1,), (1,)), ((), ())), preferred_element_type=jnp.float32
            )
            pooled[px, py] = mean.astype(jnp.bfloat16)


def level_three_conv(cells, left, right, below, above, weights, bias_values):
    extent_x, extent_y, channels, lanes = cells.shape
    depth = lanes // 2
    out_channels = weights.shape[1]
    mix = weights.transpose(0, 2, 1).reshape(27 * channels, out_channels)
    target = lax.broadcasted_iota(jnp.int32, (depth // 2, 2 * lanes), 0)
    source = lax.broadcasted_iota(jnp.int32, (depth // 2, 2 * lanes), 1) % depth // 2
    pool = jnp.where(source == target, 0.125, 0.0).astype(jnp.bfloat16)
    return pl.pallas_call(
        level_three_kernel,
        name="conv_three",
        out_shape=(
            jax.ShapeDtypeStruct((extent_x, extent_y // 2, out_channels, lanes), jnp.bfloat16),
            jax.ShapeDtypeStruct(
                (extent_x // 2, extent_y // 2, depth // 2, out_channels), jnp.bfloat16
            ),
        ),
        in_specs=[VMEM] * 8,
        out_specs=(VMEM, VMEM),
        scratch_shapes=[
            pltpu.VMEM((extent_x + 2, extent_y + 1, 3, channels, lanes), jnp.bfloat16)
        ],
    )(cells, left, right, below, above, mix, bias_values[:, None], pool)


def level_four_kernel(layers, cells, mix, bias, out, rolled):
    extent_x, rows, width = cells.shape
    for x in range(extent_x):
        value = cells[x]
        wide = value.astype(jnp.float32)
        rolled[0, x + 1] = pltpu.roll(wide, layers, 0).astype(value.dtype)
        rolled[1, x + 1] = value
        rolled[2, x + 1] = pltpu.roll(wide, rows - layers, 0).astype(value.dtype)
    for c in range(3):
        rolled[c, 0] = rolled[c, extent_x]
        rolled[c, extent_x + 1] = rolled[c, 1]
    total = jnp.zeros((extent_x * rows, out.shape[1]), jnp.float32)
    for a in range(3):
        for c in range(3):
            total = total + jnp.dot(
                rolled[c, a : a + extent_x].reshape(extent_x * rows, width),
                mix[3 * a + c],
                preferred_element_type=jnp.float32,
            )
    out[...] = leaky(total + bias[...]).astype(jnp.bfloat16)


def level_four_conv(slabs, weights, bias_values):
    extent_x, extent_y, depth, channels = slabs.shape
    layers = depth - 2
    out_channels = weights.shape[1]
    cells = jnp.concatenate([slabs[:, :, e : e + layers] for e in range(3)], axis=3)
    rows = extent_y * layers
    cells = cells.reshape(extent_x, rows, 3 * channels)
    mix = weights.transpose(0, 2, 1).reshape(9, 3 * channels, out_channels)
    out = pl.pallas_call(
        functools.partial(level_four_kernel, layers),
        name="conv_four",
        out_shape=jax.ShapeDtypeStruct((extent_x * rows, out_channels), jnp.bfloat16),
        in_specs=[VMEM] * 3,
        out_specs=VMEM,
        scratch_shapes=[pltpu.VMEM((3, extent_x + 2, rows, 3 * channels), jnp.bfloat16)],
    )(cells, mix, bias_values[None, :])
    return out.reshape(extent_x, extent_y, layers, out_channels).transpose(3, 0, 1, 2)


def shards(features, weight_two, bias_two, weight_three, bias_three, weight_four, bias_four):
    count_x, count_y = lax.axis_size("gx"), lax.axis_size("gy")
    cells = features.transpose(1, 2, 0, 3)
    left, right = shift_exchange(cells[0], cells[-1], "gx")
    low = jnp.concatenate([left[:1], cells[:, 0], right[:1]], axis=0)
    high = jnp.concatenate([left[-1:], cells[:, -1], right[-1:]], axis=0)
    below, above = pair_exchange(low, high, "gy")
    level_two, pooled = level_two_conv(cells, left, right, below, above, weight_two, bias_two)

    left, right = shift_exchange(pooled[0], pooled[-1], "gx")
    low = jnp.concatenate([left[:1], pooled[:, 0], right[:1]], axis=0)
    high = jnp.concatenate([left[-1:], pooled[:, -1], right[-1:]], axis=0)
    below, above = pair_exchange(low, high, "gy")
    level_three, coarse = level_three_conv(
        pooled, left, right, below, above, weight_three, bias_three
    )

    extent_x, extent_y, depth, channels = coarse.shape
    layers = depth // count_y
    ringed = jnp.concatenate([coarse[:, :, -1:], coarse, coarse[:, :, :1]], axis=2)
    windows = jnp.stack(
        [ringed[:, :, layers * d : layers * (d + 1) + 2] for d in range(count_y)], axis=0
    )
    windows = jnp.broadcast_to(windows, (count_x,) + windows.shape)
    windows = windows.reshape((count_x * count_y,) + windows.shape[2:])
    slabs = lax.all_to_all(windows, ("gx", "gy"), 0, 0, tiled=True)
    slabs = slabs.reshape(count_x, count_y, extent_x, extent_y, layers + 2, channels)
    slabs = slabs.transpose(0, 2, 1, 3, 4, 5).reshape(
        count_x * extent_x, count_y * extent_y, layers + 2, channels
    )
    bottleneck = level_four_conv(slabs, weight_four, bias_four)
    out_three = level_three.reshape(level_three.shape[:3] + (2, level_three.shape[3] // 2))
    out_three = out_three.transpose(2, 0, 1, 3, 4)
    out_three = out_three.reshape(out_three.shape[:2] + (-1, out_three.shape[4]))
    return level_two.transpose(2, 0, 1, 3), out_three, bottleneck


def solution(mesh):
    return jax.shard_map(
        shards,
        mesh=mesh,
        in_specs=(P(None, "gx", "gy", None), P(), P(), P(), P(), P(), P()),
        out_specs=(
            P(None, "gx", "gy", None),
            P(None, "gx", "gy", None),
            P(None, None, None, "gy"),
        ),
        check_vma=False,
    )
```

```python
import functools

import jax
import jax.numpy as jnp
from jax import lax
from jax.experimental import pallas as pl
from jax.experimental.pallas import tpu as pltpu
from jax.sharding import PartitionSpec as P

VMEM = pl.BlockSpec(memory_space=pltpu.VMEM)
BF16 = jnp.bfloat16
F32 = jnp.float32
COST = pl.CostEstimate(flops=1 << 30, transcendentals=0, bytes_accessed=1 << 20)


def leaky(t):
    return jnp.where(t >= 0, t, 0.1 * t)


def near(value):
    return pltpu.with_memory_space_constraint(value, pltpu.VMEM)


def local(shape):
    return pltpu.VMEM(shape, BF16)


def column(bias):
    count = bias.shape[1]
    return jnp.broadcast_to(bias[...], (count, count)).T[:, :1]


def shift_exchange(low, high, axis):
    count = lax.axis_size(axis)
    below = lax.ppermute(high, axis, [(i, (i + 1) % count) for i in range(count)])
    above = lax.ppermute(low, axis, [((i + 1) % count, i) for i in range(count)])
    return below, above


def pair_exchange(low, high, axis):
    count = lax.axis_size(axis)
    if count % 2:
        return shift_exchange(low, high, axis)
    even = lax.axis_index(axis) % 2 == 0
    inner = [(i, i + 1 if i % 2 == 0 else i - 1) for i in range(count)]
    outer = [(i, (i - 1) % count if i % 2 == 0 else (i + 1) % count) for i in range(count)]
    from_outer = lax.ppermute(jnp.where(even, low, high), axis, outer)
    from_inner = lax.ppermute(jnp.where(even, high, low), axis, inner)
    below = jnp.where(even, from_outer, from_inner)
    above = jnp.where(even, from_inner, from_outer)
    return below, above


def mix_two(mix, bias, pool, stacked, channels, depth):
    result = jnp.dot(mix, stacked, preferred_element_type=F32)
    result = leaky(result + bias).astype(BF16)
    answers = []
    for half in range(2):
        block = result[:, half * depth : (half + 1) * depth]
        sums = jnp.dot(block, pool, preferred_element_type=F32)
        mean = sums[:channels]
        for part in range(1, 4):
            mean = mean + sums[part * channels : (part + 1) * channels]
        answers.append((block, mean.astype(BF16)))
    return answers


def pool_two(depth):
    source = lax.broadcasted_iota(jnp.int32, (depth, depth), 0) // 2
    target = lax.broadcasted_iota(jnp.int32, (depth, depth), 1) % (depth // 2)
    return jnp.where(source == target, 0.125, 0.0).astype(BF16)


def shifts(value):
    depth = value.shape[1]
    return pltpu.roll(value, 1, 1), value, pltpu.roll(value, depth - 1, 1)


def inner_two_kernel(cells, left, right, weights, bias, out, pooled, rolled, mix):
    extent_x, extent_y, channels, depth = cells.shape
    for y in range(extent_y):
        for x in range(extent_x + 2):
            if x == 0:
                value = left[y]
            elif x == extent_x + 1:
                value = right[y]
            else:
                value = cells[x - 1, y]
            for e, turned in enumerate(shifts(value)):
                rolled[e, x, y] = turned
    blank = jnp.zeros((channels, channels), BF16)
    empty = jnp.zeros((channels, 4 * channels), BF16)
    for e in range(3):
        for dx in range(2):
            for dy in range(2):
                rows = slice((2 * dx + dy) * channels, (2 * dx + dy + 1) * channels)
                for wide_x in range(4):
                    a = wide_x - dx
                    tile = empty
                    if 0 <= a < 3:
                        taps = [weights[9 * a + 3 * c + e] for c in range(3)]
                        tile = jnp.concatenate([blank] * dy + taps + [blank] * (1 - dy), axis=1)
                    at = (4 * e + wide_x) * 4 * channels
                    mix[rows, at : at + 4 * channels] = tile
    offset = jnp.concatenate([column(bias)] * 4, axis=0)
    pool = pool_two(depth)
    matrix = mix[...]
    blocks = [(x, y) for x in range(0, extent_x, 2) for y in range(2, extent_y - 2, 2)]
    for pair in range(0, len(blocks), 2):
        both = blocks[pair : pair + 2]
        stacked = jnp.concatenate(
            [
                rolled[:, x : x + 4, y - 1 : y + 3].reshape(48 * channels, depth)
                for x, y in both
            ],
            axis=1,
        )
        answers = mix_two(matrix, offset, pool, stacked, channels, depth)
        for (x, y), (block, mean) in zip(both, answers):
            for part in range(4):
                out[x + part // 2, y - 2 + part % 2] = block[
                    part * channels : (part + 1) * channels
                ]
            pooled[x // 2, y // 2 - 1] = mean


def rim_two_kernel(rolled, below, above, inner, inner_pooled, mix, bias, out, pooled, rim):
    _, wide_x, extent_y, channels, depth = rolled.shape
    extent_x = wide_x - 2
    for x in range(wide_x):
        for side, source in enumerate((below, above)):
            for e, turned in enumerate(shifts(source[x])):
                rim[side, e, x] = turned
    offset = jnp.concatenate([column(bias)] * 4, axis=0)
    pool = pool_two(depth)
    matrix = mix[...]
    for x in range(0, extent_x, 2):
        low, high = [], []
        for e in range(3):
            for at in range(x, x + 4):
                low.append(rim[0, e, at])
                low.append(rolled[e, at, 0:3].reshape(3 * channels, depth))
                high.append(rolled[e, at, extent_y - 3 : extent_y].reshape(3 * channels, depth))
                high.append(rim[1, e, at])
        stacked = jnp.concatenate(
            [jnp.concatenate(low, axis=0), jnp.concatenate(high, axis=0)], axis=1
        )
        answers = mix_two(matrix, offset, pool, stacked, channels, depth)
        for y, (block, mean) in zip((0, extent_y - 2), answers):
            for part in range(4):
                out[x + part // 2, y + part % 2] = block[part * channels : (part + 1) * channels]
            pooled[x // 2, y // 2] = mean
    out[:, 2 : extent_y - 2] = inner[...]
    pooled[:, 1 : extent_y // 2 - 1] = inner_pooled[...]


def inner_two(cells, left, right, weights, bias):
    extent_x, extent_y, channels, depth = cells.shape
    return pl.pallas_call(
        inner_two_kernel,
        name="inner_two",
        out_shape=(
            local((extent_x, extent_y - 4, channels, depth)),
            local((extent_x // 2, extent_y // 2 - 2, channels, depth)),
            local((3, extent_x + 2, extent_y, channels, depth)),
            local((4 * channels, 48 * channels)),
        ),
        in_specs=[VMEM] * 5,
        out_specs=(VMEM,) * 4,
        cost_estimate=COST,
        compiler_params=pltpu.CompilerParams(vmem_limit_bytes=16 << 20),
    )(near(cells), near(left), near(right), near(weights), near(bias))


def rim_two(rolled, below, above, inner, inner_pooled, mix, bias):
    _, wide_x, extent_y, channels, depth = rolled.shape
    extent_x = wide_x - 2
    return pl.pallas_call(
        rim_two_kernel,
        name="rim_two",
        out_shape=(
            local((extent_x, extent_y, channels, depth)),
            local((extent_x // 2, extent_y // 2, channels, depth)),
        ),
        in_specs=[VMEM] * 7,
        out_specs=(VMEM,) * 2,
        scratch_shapes=[pltpu.VMEM((2, 3, wide_x, channels, depth), BF16)],
        cost_estimate=COST,
        compiler_params=pltpu.CompilerParams(vmem_limit_bytes=16 << 20),
    )(*map(near, (rolled, below, above, inner, inner_pooled, mix, bias)))


def three_kernel(layers, cells, left, right, below, above, mix, bias, out, windows, paired):
    extent_x, extent_y, channels, lanes = cells.shape
    depth = lanes // 2
    out_channels = mix.shape[1]
    senders, slots = windows.shape[:2]

    def place(x, y):
        if y == 0:
            return below[x]
        if y == extent_y + 1:
            return above[x]
        if x == 0:
            return left[y - 1]
        if x == extent_x + 1:
            return right[y - 1]
        return cells[x - 1, y - 1]

    first = lax.broadcasted_iota(jnp.int32, (channels, lanes), 1) < depth
    for x in range(extent_x + 2):
        turned = [shifts(place(x, y)) for y in range(extent_y + 2)]
        for y in range(extent_y + 1):
            for e in range(3):
                paired[x, y, e] = jnp.where(first, turned[y][e], turned[y + 1][e])
    offset = column(bias)
    rows = lax.broadcasted_iota(jnp.int32, (slots * 8, 2 * lanes), 0)
    layer = rows % 8
    wanted = (layers * (rows // 8) + layer + depth // 2 - 1) % (depth // 2)
    source = lax.broadcasted_iota(jnp.int32, (slots * 8, 2 * lanes), 1) % depth // 2
    pool = jnp.where((source == wanted) & (layer < layers + 2), 0.125, 0.0).astype(BF16)
    matrix = mix[...]
    for px in range(extent_x // 2):
        results = []
        for py in range(extent_y // 2):
            stacked = jnp.concatenate(
                [
                    jnp.concatenate(
                        [
                            paired[x + a, 2 * py + c].reshape(3 * channels, lanes)
                            for a in range(3)
                            for c in range(3)
                        ],
                        axis=0,
                    )
                    for x in (2 * px, 2 * px + 1)
                ],
                axis=1,
            )
            result = lax.dot_general(
                matrix, stacked, (((0,), (0,)), ((), ())), preferred_element_type=F32
            )
            result = leaky(result + offset).astype(BF16)
            out[2 * px, py] = result[:, :lanes]
            out[2 * px + 1, py] = result[:, lanes:]
            results.append(result)
        means = lax.dot_general(
            pool,
            jnp.concatenate(results, axis=0),
            (((1,), (1,)), ((), ())),
            preferred_element_type=F32,
        ).astype(BF16)
        for slot in range(slots):
            for sender in range(senders):
                windows[sender, slot, 8 * px : 8 * px + 8] = means[8 * slot : 8 * slot + 8]


def three(cells, left, right, below, above, weights, bias_values, count_x, count_y):
    extent_x, extent_y, channels, lanes = cells.shape
    depth = lanes // 2
    out_channels = weights.shape[1]
    layers = depth // 2 // count_y
    mix = weights.transpose(0, 2, 1).reshape(27 * channels, out_channels)
    return pl.pallas_call(
        functools.partial(three_kernel, layers),
        name="three",
        out_shape=(
            local((extent_x, extent_y // 2, out_channels, lanes)),
            local((count_x, count_y, extent_x // 2 * 8, extent_y // 2 * out_channels)),
        ),
        in_specs=[VMEM] * 7,
        out_specs=(VMEM, VMEM),
        scratch_shapes=[pltpu.VMEM((extent_x + 2, extent_y + 1, 3, channels, lanes), BF16)],
        cost_estimate=COST,
        compiler_params=pltpu.CompilerParams(vmem_limit_bytes=16 << 20),
    )(*map(near, (cells, left, right, below, above, mix, bias_values)))


def four_kernel(count_y, tiles, mix, bias, out, rolled):
    sources, parts, lanes = tiles.shape
    extent_x, extent_y, layers, out_channels = out.shape
    rows = count_y * 8
    inner_x = parts // 8
    half = lanes // 2
    upper = lax.broadcasted_iota(jnp.int32, (rows, lanes), 1) >= half
    for x in range(extent_x):
        start = x // inner_x * count_y
        at = x % inner_x * 8
        value = tiles[start : start + count_y, at : at + 8].reshape(rows, lanes).astype(F32)
        before = pltpu.roll(value, 8, 0)
        after = pltpu.roll(value, rows - 8, 0)
        around = pltpu.roll(jnp.where(upper, before, after), half, 1)
        whole = jnp.concatenate([value, around], axis=1)
        for e in range(3):
            turned = whole if e == 0 else pltpu.roll(whole, rows - e, 0)
            rolled[x + 1, :, e * 2 * lanes : (e + 1) * 2 * lanes] = turned.astype(BF16)
    rolled[0] = rolled[extent_x]
    rolled[extent_x + 1] = rolled[1]
    offset = jnp.concatenate([bias[...], bias[...]], axis=1)
    matrix = mix[...]
    for x in range(0, extent_x, 2):
        stacked = jnp.concatenate(
            [rolled[x + a : x + a + 2].reshape(2 * rows, 6 * lanes) for a in range(3)], axis=1
        )
        result = jnp.dot(stacked, matrix, preferred_element_type=F32)
        result = leaky(result + offset).astype(BF16)
        for dx in range(2):
            for y in range(extent_y):
                row = dx * rows + y // 2 * 8
                lane = y % 2 * out_channels
                out[x + dx, y] = result[row : row + layers, lane : lane + out_channels]


def mix_four(weights):
    channels, out_channels = weights.shape[2], weights.shape[1]
    taps = weights.transpose(0, 2, 1).reshape(3, 3, 3, channels, out_channels)
    blank = jnp.zeros_like(taps[:, 0])
    bands = [
        jnp.concatenate(pair, axis=3)
        for pair in (
            (taps[:, 1], taps[:, 0]),
            (taps[:, 2], taps[:, 1]),
            (taps[:, 0], blank),
            (blank, taps[:, 2]),
        )
    ]
    return jnp.concatenate(bands, axis=2).reshape(36 * channels, 2 * out_channels)


def four(tiles, mix, bias, extents, count_y):
    extent_x, extent_y, layers = extents
    out_channels = mix.shape[1] // 2
    return pl.pallas_call(
        functools.partial(four_kernel, count_y),
        name="four",
        out_shape=jax.ShapeDtypeStruct((extent_x, extent_y, layers, out_channels), BF16),
        in_specs=[VMEM] * 3,
        out_specs=VMEM,
        scratch_shapes=[pltpu.VMEM((extent_x + 2, count_y * 8, 6 * tiles.shape[2]), BF16)],
        cost_estimate=COST,
        compiler_params=pltpu.CompilerParams(vmem_limit_bytes=16 << 20),
    )(near(tiles), near(mix), near(bias))


def rows_of(left, cells, right):
    low = jnp.concatenate([left[:1], cells[:, 0], right[:1]], axis=0)
    high = jnp.concatenate([left[-1:], cells[:, -1], right[-1:]], axis=0)
    return low, high


def shards(features, weight_two, bias_two, weight_three, bias_three, weight_four, bias_four):
    count_x, count_y = lax.axis_size("gx"), lax.axis_size("gy")
    left, right = shift_exchange(
        features[:, 0].transpose(1, 0, 2), features[:, -1].transpose(1, 0, 2), "gx"
    )
    cells = features.transpose(1, 2, 0, 3)
    below, above = pair_exchange(*rows_of(left, cells, right), "gy")
    inner, inner_pooled, rolled, mix = inner_two(
        cells, left, right, weight_two, bias_two[None, :]
    )
    level_two, pooled = rim_two(rolled, below, above, inner, inner_pooled, mix, bias_two[None, :])

    left, right = shift_exchange(pooled[0], pooled[-1], "gx")
    below, above = pair_exchange(*rows_of(left, pooled, right), "gy")
    level_three, windows = three(
        pooled, left, right, below, above, weight_three, bias_three[None, :], count_x, count_y
    )
    slots = count_x * count_y
    tiles = lax.all_to_all(
        windows.reshape((slots,) + windows.shape[2:]), ("gx", "gy"), 0, 0, tiled=True
    )
    extent_x, extent_y, channels, depth = level_two.shape
    extents = (count_x * extent_x // 4, count_y * extent_y // 4, depth // 4 // count_y)
    bottleneck = four(tiles, mix_four(weight_four), bias_four[None, :], extents, count_y)
    out_three = level_three.reshape(level_three.shape[:3] + (2, level_three.shape[3] // 2))
    out_three = out_three.transpose(2, 0, 1, 3, 4)
    out_three = out_three.reshape(out_three.shape[:2] + (-1, out_three.shape[4]))
    return level_two.transpose(2, 0, 1, 3), out_three, bottleneck.transpose(3, 0, 1, 2)


def solution(mesh):
    return jax.shard_map(
        shards,
        mesh=mesh,
        in_specs=(P(None, "gx", "gy", None), P(), P(), P(), P(), P(), P()),
        out_specs=(
            P(None, "gx", "gy", None),
            P(None, "gx", "gy", None),
            P(None, None, None, "gy"),
        ),
        check_vma=False,
    )
```

```python
import functools

import jax
import jax.numpy as jnp
from jax import lax
from jax.experimental import pallas as pl
from jax.experimental.pallas import tpu as pltpu
from jax.sharding import PartitionSpec as P


VMEM = pl.BlockSpec(memory_space=pltpu.VMEM)
BF16 = jnp.bfloat16
F32 = jnp.float32
COST = pl.CostEstimate(flops=1 << 30, transcendentals=0, bytes_accessed=1 << 20)


def leaky(t):
    return jnp.where(t >= 0, t, 0.1 * t)


def near(value):
    return pltpu.with_memory_space_constraint(value, pltpu.VMEM)


def local(shape):
    return pltpu.VMEM(shape, BF16)


def column(bias):
    count = bias.shape[1]
    return jnp.broadcast_to(bias[...], (count, count)).T[:, :1]


def shift_exchange(low, high, axis):
    count = lax.axis_size(axis)
    below = lax.ppermute(high, axis, [(i, (i + 1) % count) for i in range(count)])
    above = lax.ppermute(low, axis, [((i + 1) % count, i) for i in range(count)])
    return below, above


def pair_exchange(low, high, axis):
    count = lax.axis_size(axis)
    if count % 2:
        far, near_rim = shift_exchange(low, high, axis)
        return near_rim, far, jnp.bool_(True)
    even = lax.axis_index(axis) % 2 == 0
    inner = [(i, i + 1 if i % 2 == 0 else i - 1) for i in range(count)]
    outer = [(i, (i - 1) % count if i % 2 == 0 else (i + 1) % count) for i in range(count)]
    far = lax.ppermute(jnp.where(even, low, high), axis, outer)
    near_rim = lax.ppermute(jnp.where(even, high, low), axis, inner)
    return near_rim, far, even


def mix_two(mix, bias, pool, stacked, channels, depth):
    result = jnp.dot(mix, stacked, preferred_element_type=F32)
    result = leaky(result + bias).astype(BF16)
    answers = []
    for half in range(result.shape[1] // depth):
        block = result[:, half * depth : (half + 1) * depth]
        sums = jnp.dot(block, pool, preferred_element_type=F32)
        mean = sums[:channels]
        for part in range(1, 4):
            mean = mean + sums[part * channels : (part + 1) * channels]
        answers.append((block, mean.astype(BF16)))
    return answers


def pool_two(depth):
    source = lax.broadcasted_iota(jnp.int32, (depth, depth), 0) // 2
    target = lax.broadcasted_iota(jnp.int32, (depth, depth), 1) % (depth // 2)
    return jnp.where(source == target, 0.125, 0.0).astype(BF16)


def shifts(value):
    depth = value.shape[1]
    return pltpu.roll(value, 1, 1), value, pltpu.roll(value, depth - 1, 1)


def inner_two_kernel(cells, left, right, weights, bias, out, pooled, rolled, mix):
    extent_x, extent_y, channels, depth = cells.shape
    for y in range(extent_y):
        for x in range(extent_x + 2):
            if x == 0:
                value = left[y]
            elif x == extent_x + 1:
                value = right[y]
            else:
                value = cells[x - 1, y]
            for e, turned in enumerate(shifts(value)):
                rolled[e, x, y] = turned
    blank = jnp.zeros((channels, channels), BF16)
    empty = jnp.zeros((channels, 4 * channels), BF16)
    for e in range(3):
        for dx in range(2):
            for dy in range(2):
                rows = slice((2 * dx + dy) * channels, (2 * dx + dy + 1) * channels)
                for wide_x in range(4):
                    a = wide_x - dx
                    tile = empty
                    if 0 <= a < 3:
                        taps = [weights[9 * a + 3 * c + e] for c in range(3)]
                        tile = jnp.concatenate([blank] * dy + taps + [blank] * (1 - dy), axis=1)
                    at = (4 * e + wide_x) * 4 * channels
                    mix[rows, at : at + 4 * channels] = tile
    offset = jnp.concatenate([column(bias)] * 4, axis=0)
    pool = pool_two(depth)
    matrix = mix[...]
    blocks = [(x, y) for x in range(0, extent_x, 2) for y in range(2, extent_y - 2, 2)]
    for pair in range(0, len(blocks), 4):
        both = blocks[pair : pair + 4]
        stacked = jnp.concatenate(
            [
                rolled[:, x : x + 4, y - 1 : y + 3].reshape(48 * channels, depth)
                for x, y in both
            ],
            axis=1,
        )
        answers = mix_two(matrix, offset, pool, stacked, channels, depth)
        for (x, y), (block, mean) in zip(both, answers):
            for part in range(4):
                out[x + part // 2, y - 2 + part % 2] = block[
                    part * channels : (part + 1) * channels
                ]
            pooled[x // 2, y // 2 - 1] = mean


def rim_two_kernel(side, rolled, halo, mix, bias, out, pooled, band):
    _, wide_x, extent_y, channels, depth = rolled.shape
    extent_x, width = wide_x - 2, halo.shape[1]
    offset = jnp.concatenate([column(bias)] * 4, axis=0)
    pool = pool_two(depth)
    matrix = mix[...]

    def fill(x):
        for row in range(width):
            for e, turned in enumerate(shifts(halo[x, row])):
                band[e, x, row] = turned

    def edge(above):
        def rows(e, x, first):
            if above:
                start = extent_y - width + first
                pieces = [rolled[e, x, start:extent_y], band[e, x, : first + 4 - width]]
            else:
                pieces = [band[e, x, first:], rolled[e, x, : first + 4 - width]]
            return [piece.reshape(-1, depth) for piece in pieces]

        for x in range(wide_x):
            fill(x)
        blocks = [(x, first) for x in range(0, extent_x, 2) for first in (0, 2)]
        for group in range(0, len(blocks), 4):
            some = blocks[group : group + 4]
            stacked = jnp.concatenate(
                [
                    jnp.concatenate(
                        [
                            piece
                            for e in range(3)
                            for at in range(x, x + 4)
                            for piece in rows(e, at, first)
                        ],
                        axis=0,
                    )
                    for x, first in some
                ],
                axis=1,
            )
            answers = mix_two(matrix, offset, pool, stacked, channels, depth)
            for (x, first), (block, mean) in zip(some, answers):
                own = (first == 0) == above
                if own:
                    for part in range(4):
                        out[x + part // 2, part % 2] = block[
                            part * channels : (part + 1) * channels
                        ]
                pooled[0 if own else 1, x // 2] = mean

    @pl.when(side[0] == 1)
    def _():
        edge(True)

    @pl.when(side[0] == 0)
    def _():
        edge(False)


def inner_two(cells, left, right, weights, bias):
    extent_x, extent_y, channels, depth = cells.shape
    return pl.pallas_call(
        inner_two_kernel,
        name="inner_two",
        out_shape=(
            local((extent_x, extent_y - 4, channels, depth)),
            local((extent_x // 2, extent_y // 2 - 2, channels, depth)),
            local((3, extent_x + 2, extent_y, channels, depth)),
            local((4 * channels, 48 * channels)),
        ),
        in_specs=[VMEM] * 5,
        out_specs=(VMEM,) * 4,
        cost_estimate=COST,
        compiler_params=pltpu.CompilerParams(vmem_limit_bytes=16 << 20),
    )(near(cells), near(left), near(right), near(weights), near(bias))


def rim_two(side, rolled, halo, mix, bias):
    _, wide_x, _, channels, depth = rolled.shape
    extent_x, width = wide_x - 2, halo.shape[1]
    return pl.pallas_call(
        rim_two_kernel,
        name="rim_two",
        out_shape=(
            local((extent_x, 2, channels, depth)),
            local((2, extent_x // 2, channels, depth)),
        ),
        in_specs=[pl.BlockSpec(memory_space=pltpu.SMEM)] + [VMEM] * 4,
        out_specs=(VMEM,) * 2,
        scratch_shapes=[pltpu.VMEM((3, wide_x, width, channels, depth), BF16)],
        cost_estimate=COST,
        compiler_params=pltpu.CompilerParams(vmem_limit_bytes=16 << 20),
    )(side, *map(near, (rolled, halo, mix, bias)))


def three_kernel(layers, cells, left, right, mix, bias, out, windows, paired):
    extent_x, wide_y, channels, lanes = cells.shape
    extent_y = wide_y - 2
    depth = lanes // 2
    senders, slots = windows.shape[:2]

    def place(x, y):
        if 0 < x < extent_x + 1:
            return cells[x - 1, y]
        both = (left if x == 0 else right)[y // 2]
        return jnp.where(first == (y % 2 == 0), both, pltpu.roll(both, depth, 1))

    first = lax.broadcasted_iota(jnp.int32, (channels, lanes), 1) < depth
    for x in range(extent_x + 2):
        turned = [shifts(place(x, y)) for y in range(extent_y + 2)]
        for y in range(extent_y + 1):
            for e in range(3):
                paired[x, y, e] = jnp.where(first, turned[y][e], turned[y + 1][e])
    offset = column(bias)
    rows = lax.broadcasted_iota(jnp.int32, (slots * 8, 2 * lanes), 0)
    layer = rows % 8
    wanted = (layers * (rows // 8) + layer + depth // 2 - 1) % (depth // 2)
    source = lax.broadcasted_iota(jnp.int32, (slots * 8, 2 * lanes), 1) % depth // 2
    pool = jnp.where((source == wanted) & (layer < layers + 2), 0.125, 0.0).astype(BF16)
    matrix = mix[...]
    for px in range(extent_x // 2):
        results = []
        for py in range(extent_y // 2):
            stacked = jnp.concatenate(
                [
                    jnp.concatenate(
                        [
                            paired[x + a, 2 * py + c].reshape(3 * channels, lanes)
                            for a in range(3)
                            for c in range(3)
                        ],
                        axis=0,
                    )
                    for x in (2 * px, 2 * px + 1)
                ],
                axis=1,
            )
            result = jnp.dot(matrix, stacked, preferred_element_type=F32)
            result = leaky(result + offset).astype(BF16)
            out[2 * px, py] = result[:, :lanes]
            out[2 * px + 1, py] = result[:, lanes:]
            results.append(result)
        means = lax.dot_general(
            pool,
            jnp.concatenate(results, axis=0),
            (((1,), (1,)), ((), ())),
            preferred_element_type=F32,
        ).astype(BF16)
        for slot in range(slots):
            for sender in range(senders):
                windows[sender, slot, 8 * px : 8 * px + 8] = means[8 * slot : 8 * slot + 8]


def three(cells, left, right, weights, bias_values, count_x, count_y):
    extent_x, wide_y, channels, lanes = cells.shape
    extent_y = wide_y - 2
    depth = lanes // 2
    out_channels = weights.shape[1]
    layers = depth // 2 // count_y
    mix = weights.transpose(1, 0, 2).reshape(out_channels, 27 * channels)
    return pl.pallas_call(
        functools.partial(three_kernel, layers),
        name="three",
        out_shape=(
            local((extent_x, extent_y // 2, out_channels, lanes)),
            local((count_x, count_y, extent_x // 2 * 8, extent_y // 2 * out_channels)),
        ),
        in_specs=[VMEM] * 5,
        out_specs=(VMEM, VMEM),
        scratch_shapes=[pltpu.VMEM((extent_x + 2, extent_y + 1, 3, channels, lanes), BF16)],
        cost_estimate=COST,
        compiler_params=pltpu.CompilerParams(vmem_limit_bytes=16 << 20),
    )(*map(near, (cells, left, right, mix, bias_values)))


def four_kernel(count_y, tiles, weights, bias, out, rolled, mix):
    _, parts, lanes = tiles.shape
    extent_x, extent_y, layers, out_channels = out.shape
    rows = count_y * 8
    inner_x = parts // 8
    half = lanes // 2
    upper = lax.broadcasted_iota(jnp.int32, (rows, lanes), 1) >= half
    short = count_y * layers
    for x in range(extent_x):
        start = x // inner_x * count_y
        at = x % inner_x * 8
        value = tiles[start : start + count_y, at : at + 8].reshape(rows, lanes).astype(F32)
        before = pltpu.roll(value, 8, 0)
        after = pltpu.roll(value, rows - 8, 0)
        around = pltpu.roll(jnp.where(upper, before, after), half, 1)
        whole = jnp.concatenate([value, around], axis=1)
        for e in range(3):
            turned = whole if e == 0 else pltpu.roll(whole, rows - e, 0)
            turned = turned.reshape(count_y, 8, 2 * lanes)[:, :layers].reshape(short, 2 * lanes)
            rolled[x + 1, :, e * 2 * lanes : (e + 1) * 2 * lanes] = turned.astype(BF16)
    rolled[0] = rolled[extent_x]
    rolled[extent_x + 1] = rolled[1]
    bands = ((1, 0), (2, 1), (0, None), (None, 2))
    for a in range(3):
        for e in range(3):
            for band, taps in enumerate(bands):
                row = ((3 * a + e) * 4 + band) * half
                for index, c in enumerate(taps):
                    lane = index * out_channels
                    if c is None:
                        tap = jnp.zeros((half, out_channels), BF16)
                    else:
                        tap = weights[9 * a + 3 * c + e]
                    mix[row : row + half, lane : lane + out_channels] = tap
    offset = jnp.concatenate([bias[...], bias[...]], axis=1)
    matrix = mix[...]
    group = min(extent_x, 4)
    for x in range(0, extent_x, group):
        stacked = jnp.concatenate(
            [rolled[x + a : x + a + group].reshape(group * short, 6 * lanes) for a in range(3)],
            axis=1,
        )
        result = jnp.dot(stacked, matrix, preferred_element_type=F32)
        result = leaky(result + offset).astype(BF16)
        for dx in range(group):
            for y in range(extent_y):
                row = dx * short + y // 2 * layers
                lane = y % 2 * out_channels
                out[x + dx, y] = result[row : row + layers, lane : lane + out_channels]


def four(tiles, weights, bias, extents, count_y):
    extent_x, extent_y, layers = extents
    _, channels, out_channels = weights.shape
    return pl.pallas_call(
        functools.partial(four_kernel, count_y),
        name="four",
        out_shape=jax.ShapeDtypeStruct((extent_x, extent_y, layers, out_channels), BF16),
        in_specs=[VMEM] * 3,
        out_specs=VMEM,
        scratch_shapes=[
            pltpu.VMEM((extent_x + 2, count_y * layers, 6 * tiles.shape[2]), BF16),
            pltpu.VMEM((36 * channels, 2 * out_channels), BF16),
        ],
        cost_estimate=COST,
        compiler_params=pltpu.CompilerParams(vmem_limit_bytes=16 << 20),
    )(near(tiles), near(weights), near(bias))


def rows_of(left, cells, right, width):
    low = jnp.concatenate([left[None, :width], cells[:, :width], right[None, :width]], axis=0)
    high = jnp.concatenate([left[None, -width:], cells[:, -width:], right[None, -width:]], axis=0)
    return low, high


def shards(features, weight_two, bias_two, weight_three, bias_three, weight_four, bias_four):
    count_x, count_y = lax.axis_size("gx"), lax.axis_size("gy")
    low, high, features = lax.optimization_barrier((features[:, 0], features[:, -1], features))
    left, right = shift_exchange(low.transpose(1, 0, 2), high.transpose(1, 0, 2), "gx")
    cells = features.transpose(1, 2, 0, 3)
    near_rim, far_rim, even = pair_exchange(*rows_of(left, cells, right, 3), "gy")
    bias = bias_two[None, :]
    inner, inner_pooled, rolled, mix = inner_two(cells, left, right, weight_two, bias)
    side = even.astype(jnp.int32)[None]
    near_out, near_pooled = rim_two(side, rolled, near_rim, mix, bias)
    far_out, far_pooled = rim_two(1 - side, rolled, far_rim, mix, bias)
    low_pooled = jnp.where(even, far_pooled, near_pooled)
    high_pooled = jnp.where(even, near_pooled, far_pooled)
    pooled = jnp.concatenate(
        [
            low_pooled[1][:, None],
            low_pooled[0][:, None],
            inner_pooled,
            high_pooled[0][:, None],
            high_pooled[1][:, None],
        ],
        axis=1,
    )
    low_out = jnp.where(even, far_out, near_out)
    high_out = jnp.where(even, near_out, far_out)
    level_two = jnp.concatenate([low_out, inner, high_out], axis=1)

    first = jnp.arange(pooled.shape[3]) < pooled.shape[3] // 2
    low, high = [jnp.where(first, face[0::2], face[1::2]) for face in (pooled[0], pooled[-1])]
    left, right = shift_exchange(low, high, "gx")
    level_three, windows = three(
        pooled, left, right, weight_three, bias_three[None, :], count_x, count_y
    )
    slots = count_x * count_y
    tiles = lax.all_to_all(
        windows.reshape((slots,) + windows.shape[2:]), ("gx", "gy"), 0, 0, tiled=True
    )
    extent_x, extent_y, _, depth = level_two.shape
    extents = (count_x * extent_x // 4, count_y * extent_y // 4, depth // 4 // count_y)
    bottleneck = four(tiles, weight_four.transpose(0, 2, 1), bias_four[None, :], extents, count_y)
    out_three = level_three.reshape(level_three.shape[:3] + (2, level_three.shape[3] // 2))
    out_three = out_three.transpose(2, 0, 1, 3, 4)
    out_three = out_three.reshape(out_three.shape[:2] + (-1, out_three.shape[4]))
    return level_two.transpose(2, 0, 1, 3), out_three, bottleneck.transpose(3, 0, 1, 2)


def solution(mesh):
    return jax.shard_map(
        shards,
        mesh=mesh,
        in_specs=(P(None, "gx", "gy", None), P(), P(), P(), P(), P(), P()),
        out_specs=(
            P(None, "gx", "gy", None),
            P(None, "gx", "gy", None),
            P(None, None, None, "gy"),
        ),
        check_vma=False,
    )
```

```python
import functools

import jax
import jax.numpy as jnp
from jax import lax
from jax.experimental import pallas as pl
from jax.experimental.pallas import tpu as pltpu
from jax.sharding import PartitionSpec as P


VMEM = pl.BlockSpec(memory_space=pltpu.VMEM)
BF16 = jnp.bfloat16
F32 = jnp.float32
COST = pl.CostEstimate(flops=1 << 30, transcendentals=0, bytes_accessed=1 << 20)


def leaky(t):
    return jnp.where(t >= 0, t, 0.1 * t)


def near_memory(value):
    return pltpu.with_memory_space_constraint(value, pltpu.VMEM)


def local(shape):
    return pltpu.VMEM(shape, BF16)


def column(bias):
    count = bias.shape[1]
    return jnp.broadcast_to(bias[...], (count, count)).T[:, :1]


def shift_exchange(low, high, axis):
    count = lax.axis_size(axis)
    below = lax.ppermute(high, axis, [(i, (i + 1) % count) for i in range(count)])
    above = lax.ppermute(low, axis, [((i + 1) % count, i) for i in range(count)])
    return below, above


def pairings(axis):
    count = lax.axis_size(axis)
    near = [(i, i + 1 if i % 2 == 0 else i - 1) for i in range(count)]
    far = [(i, (i - 1) % count if i % 2 == 0 else (i + 1) % count) for i in range(count)]
    return near, far


def mix_two(mix, bias, pool, stacked, channels, depth):
    result = jnp.dot(mix, stacked, preferred_element_type=F32)
    result = leaky(result + bias).astype(BF16)
    answers = []
    for half in range(result.shape[1] // depth):
        block = result[:, half * depth : (half + 1) * depth]
        sums = jnp.dot(block, pool, preferred_element_type=F32)
        mean = sums[:channels]
        for part in range(1, 4):
            mean = mean + sums[part * channels : (part + 1) * channels]
        answers.append((block, mean.astype(BF16)))
    return answers


def pool_two(depth):
    source = lax.broadcasted_iota(jnp.int32, (depth, depth), 0) // 2
    target = lax.broadcasted_iota(jnp.int32, (depth, depth), 1) % (depth // 2)
    return jnp.where(source == target, 0.125, 0.0).astype(BF16)


def shifts(value):
    depth = value.shape[1]
    return pltpu.roll(value, 1, 1), value, pltpu.roll(value, depth - 1, 1)


def mix_kernel(flip, weights, *refs):
    count = len(refs) // 2
    mix = refs[count]
    for source, target in zip(refs[:count], refs[count + 1 :]):
        target[...] = source[...]
    channels = weights.shape[1]
    blank = jnp.zeros((channels, channels), BF16)
    empty = jnp.zeros((channels, 4 * channels), BF16)
    turn = flip[0]
    for e in range(3):
        for a in range(3):
            taps = [weights[9 * a + e + 3 * (c + turn * (2 - 2 * c))] for c in range(3)]
            for dy in range(2):
                tile = jnp.concatenate([blank] * dy + taps + [blank] * (1 - dy), axis=1)
                for dx in range(2):
                    row = (2 * dx + dy) * channels
                    at = (4 * e + a + dx) * 4 * channels
                    mix[row : row + channels, at : at + 4 * channels] = tile
        for dy in range(2):
            for dx in range(2):
                row = (2 * dx + dy) * channels
                at = (4 * e + 3 * (1 - dx)) * 4 * channels
                mix[row : row + channels, at : at + 4 * channels] = empty


def store_block(block, target, x, y, turn, channels):
    for part in range(4):
        dx, dy = part // 2, part % 2
        target[x + dx, y + dy + turn * (1 - 2 * dy)] = block[
            part * channels : (part + 1) * channels
        ]


def frames(blocks):
    return sorted({at for start in blocks for at in range(start, start + 4)})


def main_two(blocks, fetch, extent_y, mix, bias, turn, out, pooled, edge, rolled):
    width, channels, depth = edge.shape[2:]
    columns = frames(blocks)
    for slot, x in enumerate(columns):
        for y in range(extent_y + width):
            for e, turned in enumerate(shifts(fetch(x, y))):
                if y < width:
                    edge[e, slot, y] = turned
                if y:
                    rolled[e, slot, y - 1] = turned
    offset = jnp.concatenate([column(bias)] * 4, axis=0)
    pool = pool_two(depth)
    matrix = mix[...]
    for index, x in enumerate(blocks):
        slot = columns.index(x)
        rows = list(range(2, extent_y + 1, 2))
        stacked = jnp.concatenate(
            [
                rolled[:, slot : slot + 4, y - 2 : y + 2].reshape(48 * channels, depth)
                for y in rows
            ],
            axis=1,
        )
        answers = mix_two(matrix, offset, pool, stacked, channels, depth)
        for y, (block, mean) in zip(rows, answers):
            if y < extent_y:
                at = y - 2 + turn * (extent_y - 2 * y)
                store_block(block, out, 2 * index, at, turn, channels)
            pooled[index, y // 2 - 1 + turn * (extent_y // 2 + 1 - y)] = mean


def mirrored(y, extent_y, turn):
    return y + turn * (extent_y - 1 - 2 * y) if y < extent_y else y


def center_two_kernel(flip, cells, near, mix, bias, out, pooled, edge, rolled):
    extent_x, extent_y = cells.shape[:2]

    def fetch(x, y):
        if y < extent_y:
            return cells[x - 1, mirrored(y, extent_y, flip[0])]
        return near[x - 1, y - extent_y]

    blocks = list(range(2, extent_x - 2, 2))
    main_two(blocks, fetch, extent_y, mix, bias, flip[0], out, pooled, edge, rolled)


def sides_two_kernel(flip, cells, near, left, right, mix, bias, out, pooled, edge, rolled):
    extent_x, extent_y = cells.shape[:2]

    def fetch(x, y):
        at = mirrored(y, extent_y, flip[0])
        if x == 0:
            return left[at]
        if x == extent_x + 1:
            return right[at]
        if y < extent_y:
            return cells[x - 1, at]
        return near[x - 1, y - extent_y]

    blocks = [0, extent_x - 2]
    main_two(blocks, fetch, extent_y, mix, bias, flip[0], out, pooled, edge, rolled)


def far_two(blocks, fetch, edge, mix, bias, turn, out, pooled, shift, rim):
    _, _, width, channels, depth = edge.shape
    columns = frames(blocks)
    for x in columns:
        for row in range(width):
            for e, turned in enumerate(shifts(fetch(x, row))):
                rim[e, x, width - 1 - row] = turned
    offset = jnp.concatenate([column(bias)] * 4, axis=0)
    pool = pool_two(depth)
    starts = [(x, first) for x in blocks for first in (0, 2)]
    stacked = jnp.concatenate(
        [
            jnp.concatenate(
                [
                    piece.reshape(-1, depth)
                    for e in range(3)
                    for at in range(x, x + 4)
                    for piece in (
                        rim[e, at, first:],
                        edge[e, columns.index(at), : first + 4 - width],
                    )
                ],
                axis=0,
            )
            for x, first in starts
        ],
        axis=1,
    )
    answers = mix_two(mix[...], offset, pool, stacked, channels, depth)
    for (x, first), (block, mean) in zip(starts, answers):
        if first:
            store_block(block, out, x - shift, 0, turn, channels)
        own = first // 2
        pooled[(x - shift) // 2, own + turn * (1 - 2 * own)] = mean


def middle_two_kernel(flip, far, edge, mix, bias, out, pooled, rim):
    extent_x = far.shape[0]
    far_two(
        list(range(2, extent_x - 2, 2)),
        lambda x, row: far[x - 1, row],
        edge,
        mix,
        bias,
        flip[0],
        out,
        pooled,
        2,
        rim,
    )


def corner_two_kernel(
    flip, far, left, right, edge, mix, bias, middle, middle_pooled, center_pooled, sides_pooled,
    out, pooled, low, high, rim, means,
):
    extent_x = far.shape[0]
    turn = flip[0]

    def fetch(x, row):
        if x == 0:
            return left[row]
        if x == extent_x + 1:
            return right[row]
        return far[x - 1, row]

    far_two([0, extent_x - 2], fetch, edge, mix, bias, turn, out, means, 0, rim)
    out[2 : extent_x - 2] = middle[...]
    means[1 : extent_x // 2 - 1] = middle_pooled[...]
    rest = center_pooled.shape[1]
    pooled[:, pl.ds(turn * rest, 2)] = means[...]
    main = pl.ds(2 - 2 * turn, rest)
    last = extent_x // 2 - 1
    pooled[0:1, main] = sides_pooled[0:1]
    pooled[1:last, main] = center_pooled[...]
    pooled[last : last + 1, main] = sides_pooled[1:2]
    channels, depth = low.shape[1:]
    first = lax.broadcasted_iota(jnp.int32, (channels, depth), 1) < depth // 2
    for target, x in ((low, 0), (high, extent_x // 2 - 1)):
        for pair in range(target.shape[0]):
            target[pair] = jnp.where(first, pooled[x, 2 * pair], pooled[x, 2 * pair + 1])


SCALAR = pl.BlockSpec(memory_space=pltpu.SMEM)


def kernel_call(body, flip, operands, results, scratch):
    return pl.pallas_call(
        body,
        out_shape=tuple(
            local(result) if isinstance(result, tuple) else result for result in results
        ),
        in_specs=[SCALAR] + [VMEM] * len(operands),
        out_specs=(VMEM,) * len(results),
        scratch_shapes=[pltpu.VMEM(shape, BF16) for shape in scratch],
        cost_estimate=COST,
        compiler_params=pltpu.CompilerParams(vmem_limit_bytes=16 << 20),
    )(flip, *map(near_memory, operands))


def three_kernel(layers, cells, left, right, mix, bias, out, windows, paired):
    extent_x, wide_y, channels, lanes = cells.shape
    extent_y = wide_y - 2
    depth = lanes // 2
    senders, slots = windows.shape[:2]

    def place(x, y):
        if 0 < x < extent_x + 1:
            return cells[x - 1, y]
        both = (left if x == 0 else right)[y // 2]
        return jnp.where(first == (y % 2 == 0), both, pltpu.roll(both, depth, 1))

    first = lax.broadcasted_iota(jnp.int32, (channels, lanes), 1) < depth
    for x in range(extent_x + 2):
        turned = [shifts(place(x, y)) for y in range(extent_y + 2)]
        for y in range(extent_y + 1):
            for e in range(3):
                paired[x, y, e] = jnp.where(first, turned[y][e], turned[y + 1][e])
    offset = column(bias)
    rows = lax.broadcasted_iota(jnp.int32, (slots * 8, 2 * lanes), 0)
    layer = rows % 8
    wanted = (layers * (rows // 8) + layer + depth // 2 - 1) % (depth // 2)
    source = lax.broadcasted_iota(jnp.int32, (slots * 8, 2 * lanes), 1) % depth // 2
    pool = jnp.where((source == wanted) & (layer < layers + 2), 0.125, 0.0).astype(BF16)
    matrix = mix[...]
    for px in range(extent_x // 2):
        results = []
        for py in range(extent_y // 2):
            stacked = jnp.concatenate(
                [
                    jnp.concatenate(
                        [
                            paired[x + a, 2 * py + c].reshape(3 * channels, lanes)
                            for a in range(3)
                            for c in range(3)
                        ],
                        axis=0,
                    )
                    for x in (2 * px, 2 * px + 1)
                ],
                axis=1,
            )
            result = jnp.dot(matrix, stacked, preferred_element_type=F32)
            result = leaky(result + offset).astype(BF16)
            out[2 * px, py] = result[:, :lanes]
            out[2 * px + 1, py] = result[:, lanes:]
            results.append(result)
        means = lax.dot_general(
            pool,
            jnp.concatenate(results, axis=0),
            (((1,), (1,)), ((), ())),
            preferred_element_type=F32,
        ).astype(BF16)
        for slot in range(slots):
            for sender in range(senders):
                windows[sender, slot, 8 * px : 8 * px + 8] = means[8 * slot : 8 * slot + 8]


def three(cells, left, right, weights, bias_values, count_x, count_y):
    extent_x, wide_y, channels, lanes = cells.shape
    extent_y = wide_y - 2
    depth = lanes // 2
    out_channels = weights.shape[1]
    layers = depth // 2 // count_y
    mix = weights.transpose(1, 0, 2).reshape(out_channels, 27 * channels)
    return pl.pallas_call(
        functools.partial(three_kernel, layers),
        name="three",
        out_shape=(
            local((extent_x, extent_y // 2, out_channels, lanes)),
            local((count_x, count_y, extent_x // 2 * 8, extent_y // 2 * out_channels)),
        ),
        in_specs=[VMEM] * 5,
        out_specs=(VMEM, VMEM),
        scratch_shapes=[pltpu.VMEM((extent_x + 2, extent_y + 1, 3, channels, lanes), BF16)],
        cost_estimate=COST,
        compiler_params=pltpu.CompilerParams(vmem_limit_bytes=16 << 20),
    )(*map(near_memory, (cells, left, right, mix, bias_values)))


def four_kernel(count_y, tiles, weights, bias, out, rolled, mix):
    _, parts, lanes = tiles.shape
    extent_x, extent_y, layers, out_channels = out.shape
    rows = count_y * 8
    inner_x = parts // 8
    half = lanes // 2
    upper = lax.broadcasted_iota(jnp.int32, (rows, lanes), 1) >= half
    short = count_y * layers
    for x in range(extent_x):
        start = x // inner_x * count_y
        at = x % inner_x * 8
        value = tiles[start : start + count_y, at : at + 8].reshape(rows, lanes).astype(F32)
        before = pltpu.roll(value, 8, 0)
        after = pltpu.roll(value, rows - 8, 0)
        around = pltpu.roll(jnp.where(upper, before, after), half, 1)
        whole = jnp.concatenate([value, around], axis=1)
        for e in range(3):
            turned = whole if e == 0 else pltpu.roll(whole, rows - e, 0)
            turned = turned.reshape(count_y, 8, 2 * lanes)[:, :layers].reshape(short, 2 * lanes)
            rolled[x + 1, :, e * 2 * lanes : (e + 1) * 2 * lanes] = turned.astype(BF16)
    rolled[0] = rolled[extent_x]
    rolled[extent_x + 1] = rolled[1]
    bands = ((1, 0), (2, 1), (0, None), (None, 2))
    for a in range(3):
        for e in range(3):
            for band, taps in enumerate(bands):
                row = ((3 * a + e) * 4 + band) * half
                for index, c in enumerate(taps):
                    lane = index * out_channels
                    if c is None:
                        tap = jnp.zeros((half, out_channels), BF16)
                    else:
                        tap = weights[9 * a + 3 * c + e]
                    mix[row : row + half, lane : lane + out_channels] = tap
    offset = jnp.concatenate([bias[...], bias[...]], axis=1)
    matrix = mix[...]
    group = min(extent_x, 4)
    for x in range(0, extent_x, group):
        stacked = jnp.concatenate(
            [rolled[x + a : x + a + group].reshape(group * short, 6 * lanes) for a in range(3)],
            axis=1,
        )
        result = jnp.dot(stacked, matrix, preferred_element_type=F32)
        result = leaky(result + offset).astype(BF16)
        for dx in range(group):
            for y in range(extent_y):
                row = dx * short + y // 2 * layers
                lane = y % 2 * out_channels
                out[x + dx, y] = result[row : row + layers, lane : lane + out_channels]


def four(tiles, weights, bias, extents, count_y):
    extent_x, extent_y, layers = extents
    _, channels, out_channels = weights.shape
    return pl.pallas_call(
        functools.partial(four_kernel, count_y),
        name="four",
        out_shape=jax.ShapeDtypeStruct((extent_x, extent_y, layers, out_channels), BF16),
        in_specs=[VMEM] * 3,
        out_specs=VMEM,
        scratch_shapes=[
            pltpu.VMEM((extent_x + 2, count_y * layers, 6 * tiles.shape[2]), BF16),
            pltpu.VMEM((36 * channels, 2 * out_channels), BF16),
        ],
        cost_estimate=COST,
        compiler_params=pltpu.CompilerParams(vmem_limit_bytes=16 << 20),
    )(near_memory(tiles), near_memory(weights), near_memory(bias))


def shards(features, weight_two, bias_two, weight_three, bias_three, weight_four, bias_four):
    count_x, count_y = lax.axis_size("gx"), lax.axis_size("gy")
    width = 3
    cells = features.transpose(1, 2, 0, 3)
    extent_x, extent_y, channels, depth = cells.shape
    even = lax.axis_index("gy") % 2 == 0
    flip = 1 - even.astype(jnp.int32)[None]
    head, tail = cells[:, :width], cells[:, : -width - 1 : -1]
    near_pairs, far_pairs = pairings("gy")
    far = lax.ppermute(jnp.where(even, head, tail), "gy", far_pairs)
    near = lax.ppermute(jnp.where(even, tail, head), "gy", near_pairs)
    left, right = shift_exchange(
        jnp.concatenate([cells[0], near[0]], axis=0),
        jnp.concatenate([cells[-1], near[-1]], axis=0),
        "gx",
    )
    far_left, far_right = shift_exchange(far[0], far[-1], "gx")
    biases = [bias[None, :] for bias in (bias_two, bias_three, bias_four)]
    mix, bias, bias_three, bias_four = kernel_call(
        mix_kernel,
        flip,
        [weight_two, *biases],
        [local((4 * channels, 48 * channels))] + [pltpu.VMEM(row.shape, F32) for row in biases],
        [],
    )
    rest = extent_y // 2
    deep = extent_y + width - 1

    def main_call(body, name, operands, blocks):
        read = 2 * blocks + 2 if name == "center_two" else 8
        return kernel_call(
            body,
            flip,
            [cells, near, *operands, mix, bias],
            [
                (2 * blocks, extent_y - 2, channels, depth),
                (blocks, rest, channels, depth),
                (3, read, width, channels, depth),
            ],
            [(3, read, deep, channels, depth)],
        )

    center, center_pooled, center_edge = main_call(
        center_two_kernel, "center_two", [], extent_x // 2 - 2
    )
    sides, sides_pooled, sides_edge = main_call(
        sides_two_kernel, "sides_two", [left, right], 2
    )
    rim = (3, extent_x + 2, width, channels, depth)
    middle, middle_pooled = kernel_call(
        middle_two_kernel,
        flip,
        [far, center_edge, mix, bias],
        [(extent_x - 4, 2, channels, depth), (extent_x // 2 - 2, 2, channels, depth)],
        [rim],
    )
    far_out, pooled, low, high = kernel_call(
        corner_two_kernel,
        flip,
        [
            far, far_left, far_right, sides_edge, mix, bias,
            middle, middle_pooled, center_pooled, sides_pooled,
        ],
        [
            (extent_x, 2, channels, depth),
            (extent_x // 2, rest + 2, channels, depth),
            (rest // 2 + 1, channels, depth),
            (rest // 2 + 1, channels, depth),
        ],
        [rim, (extent_x // 2, 2, channels, depth)],
    )
    main = jnp.concatenate([sides[:2], center, sides[2:]], axis=0)
    level_two = jnp.where(
        even,
        jnp.concatenate([far_out, main], axis=1),
        jnp.concatenate([main, far_out], axis=1),
    ).transpose(2, 0, 1, 3)

    left, right = shift_exchange(low, high, "gx")
    level_three, windows = three(
        pooled, left, right, weight_three, bias_three, count_x, count_y
    )
    slots = count_x * count_y
    tiles = lax.all_to_all(
        windows.reshape((slots,) + windows.shape[2:]), ("gx", "gy"), 0, 0, tiled=True
    )
    extents = (count_x * extent_x // 4, count_y * extent_y // 4, depth // 4 // count_y)
    bottleneck = four(tiles, weight_four.transpose(0, 2, 1), bias_four, extents, count_y)
    out_three = level_three.reshape(level_three.shape[:3] + (2, level_three.shape[3] // 2))
    out_three = out_three.transpose(2, 0, 1, 3, 4)
    out_three = out_three.reshape(out_three.shape[:2] + (-1, out_three.shape[4]))
    return level_two, out_three, bottleneck.transpose(3, 0, 1, 2)


def solution(mesh):
    return jax.shard_map(
        shards,
        mesh=mesh,
        in_specs=(P(None, "gx", "gy", None), P(), P(), P(), P(), P(), P()),
        out_specs=(
            P(None, "gx", "gy", None),
            P(None, "gx", "gy", None),
            P(None, None, None, "gy"),
        ),
        check_vma=False,
    )
```

```python
import functools

import jax
import jax.numpy as jnp
from jax import lax
from jax.experimental import pallas as pl
from jax.experimental.pallas import tpu as pltpu
from jax.sharding import PartitionSpec as P


VMEM = pl.BlockSpec(memory_space=pltpu.VMEM)
BF16 = jnp.bfloat16
F32 = jnp.float32
SCALAR = pl.BlockSpec(memory_space=pltpu.SMEM)
COST = pl.CostEstimate(flops=1 << 30, transcendentals=0, bytes_accessed=1 << 20)


def leaky(t):
    return jnp.where(t >= 0, t, 0.1 * t)


def near_memory(value):
    return pltpu.with_memory_space_constraint(value, pltpu.VMEM)


def local(shape):
    return pltpu.VMEM(shape, BF16)


def column(bias):
    count = bias.shape[1]
    return jnp.broadcast_to(bias[...], (count, count)).T[:, :1]


def shift_exchange(low, high, axis):
    count = lax.axis_size(axis)
    below = lax.ppermute(high, axis, [(i, (i + 1) % count) for i in range(count)])
    above = lax.ppermute(low, axis, [((i + 1) % count, i) for i in range(count)])
    return below, above


def pairings(axis):
    count = lax.axis_size(axis)
    near = [(i, i + 1 if i % 2 == 0 else i - 1) for i in range(count)]
    far = [(i, (i - 1) % count if i % 2 == 0 else (i + 1) % count) for i in range(count)]
    return near, far


def mix_two(mix, bias, pool, stacked, channels, depth):
    result = jnp.dot(mix, stacked, preferred_element_type=F32)
    result = leaky(result + bias).astype(BF16)
    answers = []
    for half in range(result.shape[1] // depth):
        block = result[:, half * depth : (half + 1) * depth]
        sums = jnp.dot(block, pool, preferred_element_type=F32)
        mean = sums[:channels]
        for part in range(1, 4):
            mean = mean + sums[part * channels : (part + 1) * channels]
        answers.append((block, mean.astype(BF16)))
    return answers


def pool_two(depth):
    source = lax.broadcasted_iota(jnp.int32, (depth, depth), 0) // 2
    target = lax.broadcasted_iota(jnp.int32, (depth, depth), 1) % (depth // 2)
    return jnp.where(source == target, 0.125, 0.0).astype(BF16)


def shifts(value):
    depth = value.shape[1]
    return pltpu.roll(value, 1, 1), value, pltpu.roll(value, depth - 1, 1)


def split_kernel(flip, features, cells, head, tail, parts, arrived):
    _, extent_y = cells.shape[:2]
    count, _, step = parts.shape[:3]
    turn = flip[0]
    copies = [
        pltpu.make_async_copy(
            features.at[:, pl.ds(part * step, step)], parts.at[part], arrived.at[part]
        )
        for part in range(count)
    ]
    for copy in copies:
        copy.start()
    for part in range(count):
        copies[part].wait()
        for index in range(step):
            x = part * step + index
            cells[x] = jnp.swapaxes(parts[part, :, index], 0, 1)
            for row in range(head.shape[1]):
                head[x, row] = cells[x, mirrored(row, extent_y, turn)]
                tail[x, row] = cells[x, mirrored(extent_y - 1 - row, extent_y, turn)]


def split(flip, features, width):
    channels, extent_x, extent_y, depth = features.shape
    step = 2
    count = extent_x // step
    return pl.pallas_call(
        split_kernel,
        name="split",
        out_shape=(
            local((extent_x, extent_y, channels, depth)),
            local((extent_x, width, channels, depth)),
            local((extent_x, width, channels, depth)),
        ),
        in_specs=[SCALAR, pl.BlockSpec(memory_space=pl.ANY)],
        out_specs=(VMEM,) * 3,
        scratch_shapes=[
            pltpu.VMEM((count, channels, step, extent_y, depth), BF16),
            pltpu.SemaphoreType.DMA((count,)),
        ],
        cost_estimate=COST,
        compiler_params=pltpu.CompilerParams(vmem_limit_bytes=16 << 20),
    )(flip, pltpu.with_memory_space_constraint(features, pltpu.HBM))


def mix_kernel(flip, weights, *refs):
    count = len(refs) // 2
    mix = refs[count]
    for source, target in zip(refs[:count], refs[count + 1 :]):
        target[...] = source[...]
    channels = weights.shape[1]
    blank = jnp.zeros((channels, channels), BF16)
    empty = jnp.zeros((channels, 4 * channels), BF16)
    turn = flip[0]
    for e in range(3):
        for a in range(3):
            taps = [weights[9 * a + e + 3 * (c + turn * (2 - 2 * c))] for c in range(3)]
            for dy in range(2):
                tile = jnp.concatenate([blank] * dy + taps + [blank] * (1 - dy), axis=1)
                for dx in range(2):
                    row = (2 * dx + dy) * channels
                    at = (4 * e + a + dx) * 4 * channels
                    mix[row : row + channels, at : at + 4 * channels] = tile
        for dy in range(2):
            for dx in range(2):
                row = (2 * dx + dy) * channels
                at = (4 * e + 3 * (1 - dx)) * 4 * channels
                mix[row : row + channels, at : at + 4 * channels] = empty


def store_block(block, target, x, y, turn, channels):
    for part in range(4):
        dx, dy = part // 2, part % 2
        target[x + dx, y + dy + turn * (1 - 2 * dy)] = block[
            part * channels : (part + 1) * channels
        ]


def frames(blocks):
    return sorted({at for start in blocks for at in range(start, start + 4)})


def main_two(blocks, fetch, extent_y, mix, bias, turn, out, pooled, edge, rolled):
    width, channels, depth = edge.shape[2:]
    columns = frames(blocks)
    for slot, x in enumerate(columns):
        for y in range(extent_y + width):
            for e, turned in enumerate(shifts(fetch(x, y))):
                if y < width:
                    edge[e, slot, y] = turned
                if y:
                    rolled[e, slot, y - 1] = turned
    offset = jnp.concatenate([column(bias)] * 4, axis=0)
    pool = pool_two(depth)
    matrix = mix[...]
    for index, x in enumerate(blocks):
        slot = columns.index(x)
        rows = list(range(2, extent_y + 1, 2))
        stacked = jnp.concatenate(
            [
                rolled[:, slot : slot + 4, y - 2 : y + 2].reshape(48 * channels, depth)
                for y in rows
            ],
            axis=1,
        )
        answers = mix_two(matrix, offset, pool, stacked, channels, depth)
        for y, (block, mean) in zip(rows, answers):
            if y < extent_y:
                at = y - 2 + turn * (extent_y - 2 * y)
                store_block(block, out, 2 * index, at, turn, channels)
            pooled[index, y // 2 - 1 + turn * (extent_y // 2 + 1 - y)] = mean


def mirrored(y, extent_y, turn):
    return y + turn * (extent_y - 1 - 2 * y) if y < extent_y else y


def center_two_kernel(flip, cells, near, mix, bias, out, pooled, edge, rolled):
    extent_x, extent_y = cells.shape[:2]

    def fetch(x, y):
        if y < extent_y:
            return cells[x - 1, mirrored(y, extent_y, flip[0])]
        return near[x - 1, y - extent_y]

    blocks = list(range(2, extent_x - 2, 2))
    main_two(blocks, fetch, extent_y, mix, bias, flip[0], out, pooled, edge, rolled)


def sides_two_kernel(flip, cells, near, left, right, mix, bias, out, pooled, edge, rolled):
    extent_x, extent_y = cells.shape[:2]

    def fetch(x, y):
        at = mirrored(y, extent_y, flip[0])
        if x == 0:
            return left[at]
        if x == extent_x + 1:
            return right[at]
        if y < extent_y:
            return cells[x - 1, at]
        return near[x - 1, y - extent_y]

    blocks = [0, extent_x - 2]
    main_two(blocks, fetch, extent_y, mix, bias, flip[0], out, pooled, edge, rolled)


def far_two(blocks, fetch, edge, mix, bias, turn, out, pooled, shift, rim):
    _, _, width, channels, depth = edge.shape
    columns = frames(blocks)
    for x in columns:
        for row in range(width):
            for e, turned in enumerate(shifts(fetch(x, row))):
                rim[e, x, width - 1 - row] = turned
    offset = jnp.concatenate([column(bias)] * 4, axis=0)
    pool = pool_two(depth)
    starts = [(x, first) for x in blocks for first in (0, 2)]
    stacked = jnp.concatenate(
        [
            jnp.concatenate(
                [
                    piece.reshape(-1, depth)
                    for e in range(3)
                    for at in range(x, x + 4)
                    for piece in (
                        rim[e, at, first:],
                        edge[e, columns.index(at), : first + 4 - width],
                    )
                ],
                axis=0,
            )
            for x, first in starts
        ],
        axis=1,
    )
    answers = mix_two(mix[...], offset, pool, stacked, channels, depth)
    for (x, first), (block, mean) in zip(starts, answers):
        if first:
            store_block(block, out, x - shift, 0, turn, channels)
        own = first // 2
        pooled[(x - shift) // 2, own + turn * (1 - 2 * own)] = mean


def middle_two_kernel(flip, far, edge, mix, bias, out, pooled, rim):
    extent_x = far.shape[0]
    far_two(
        list(range(2, extent_x - 2, 2)),
        lambda x, row: far[x - 1, row],
        edge,
        mix,
        bias,
        flip[0],
        out,
        pooled,
        2,
        rim,
    )


def corner_two_kernel(
    flip, far, left, right, edge, mix, bias, middle, middle_pooled, center_pooled, sides_pooled,
    out, pooled, low, high, rim, means,
):
    extent_x = far.shape[0]
    turn = flip[0]

    def fetch(x, row):
        if x == 0:
            return left[row]
        if x == extent_x + 1:
            return right[row]
        return far[x - 1, row]

    far_two([0, extent_x - 2], fetch, edge, mix, bias, turn, out, means, 0, rim)
    out[2 : extent_x - 2] = middle[...]
    means[1 : extent_x // 2 - 1] = middle_pooled[...]
    rest = center_pooled.shape[1]
    pooled[:, pl.ds(turn * rest, 2)] = means[...]
    main = pl.ds(2 - 2 * turn, rest)
    last = extent_x // 2 - 1
    pooled[0:1, main] = sides_pooled[0:1]
    pooled[1:last, main] = center_pooled[...]
    pooled[last : last + 1, main] = sides_pooled[1:2]
    channels, depth = low.shape[1:]
    first = lax.broadcasted_iota(jnp.int32, (channels, depth), 1) < depth // 2
    for target, x in ((low, 0), (high, extent_x // 2 - 1)):
        for pair in range(target.shape[0]):
            target[pair] = jnp.where(first, pooled[x, 2 * pair], pooled[x, 2 * pair + 1])


def kernel_call(body, flip, operands, results, scratch):
    return pl.pallas_call(
        body,
        out_shape=tuple(
            local(result) if isinstance(result, tuple) else result for result in results
        ),
        in_specs=[SCALAR] + [VMEM] * len(operands),
        out_specs=(VMEM,) * len(results),
        scratch_shapes=[pltpu.VMEM(shape, BF16) for shape in scratch],
        cost_estimate=COST,
        compiler_params=pltpu.CompilerParams(vmem_limit_bytes=16 << 20),
    )(flip, *map(near_memory, operands))


def store_two_kernel(flip, far, center, sides, out, rows):
    extent_x = far.shape[0]
    extent_y = out.shape[2]
    turn = flip[0]
    for x in range(extent_x):
        if 2 <= x < extent_x - 2:
            main = center[x - 2]
        else:
            main = sides[x if x < 2 else x - extent_x + 4]
        rows[x, pl.ds(turn * (extent_y - 2), 2)] = far[x]
        rows[x, pl.ds(2 - 2 * turn, extent_y - 2)] = main
        out[:, x] = jnp.swapaxes(rows[x], 0, 1)


def store_two(flip, far, center, sides):
    extent_x, _, channels, depth = far.shape
    extent_y = center.shape[1] + 2
    return pl.pallas_call(
        store_two_kernel,
        name="store_two",
        out_shape=jax.ShapeDtypeStruct((channels, extent_x, extent_y, depth), BF16),
        in_specs=[SCALAR] + [VMEM] * 3,
        out_specs=VMEM,
        scratch_shapes=[pltpu.VMEM((extent_x, extent_y, channels, depth), BF16)],
        cost_estimate=COST,
        compiler_params=pltpu.CompilerParams(vmem_limit_bytes=16 << 20),
    )(flip, *map(near_memory, (far, center, sides)))


def three_kernel(layers, cells, left, right, mix, bias, out, windows, paired):
    extent_x, wide_y, channels, lanes = cells.shape
    extent_y = wide_y - 2
    depth = lanes // 2
    senders, slots = windows.shape[:2]

    def place(x, y):
        if 0 < x < extent_x + 1:
            return cells[x - 1, y]
        both = (left if x == 0 else right)[y // 2]
        return jnp.where(first == (y % 2 == 0), both, pltpu.roll(both, depth, 1))

    first = lax.broadcasted_iota(jnp.int32, (channels, lanes), 1) < depth
    for x in range(extent_x + 2):
        turned = [shifts(place(x, y)) for y in range(extent_y + 2)]
        for y in range(extent_y + 1):
            for e in range(3):
                paired[x, y, e] = jnp.where(first, turned[y][e], turned[y + 1][e])
    offset = column(bias)
    rows = lax.broadcasted_iota(jnp.int32, (slots * 8, 2 * lanes), 0)
    layer = rows % 8
    wanted = (layers * (rows // 8) + layer + depth // 2 - 1) % (depth // 2)
    source = lax.broadcasted_iota(jnp.int32, (slots * 8, 2 * lanes), 1) % depth // 2
    pool = jnp.where((source == wanted) & (layer < layers + 2), 0.125, 0.0).astype(BF16)
    matrix = mix[...]
    for px in range(extent_x // 2):
        results = []
        for py in range(extent_y // 2):
            stacked = jnp.concatenate(
                [
                    jnp.concatenate(
                        [
                            paired[x + a, 2 * py + c].reshape(3 * channels, lanes)
                            for a in range(3)
                            for c in range(3)
                        ],
                        axis=0,
                    )
                    for x in (2 * px, 2 * px + 1)
                ],
                axis=1,
            )
            result = jnp.dot(matrix, stacked, preferred_element_type=F32)
            result = leaky(result + offset).astype(BF16)
            out[2 * px, py] = result[:, :lanes]
            out[2 * px + 1, py] = result[:, lanes:]
            results.append(result)
        means = lax.dot_general(
            pool,
            jnp.concatenate(results, axis=0),
            (((1,), (1,)), ((), ())),
            preferred_element_type=F32,
        ).astype(BF16)
        for slot in range(slots):
            for sender in range(senders):
                windows[sender, slot, 8 * px : 8 * px + 8] = means[8 * slot : 8 * slot + 8]


def three(cells, left, right, weights, bias_values, count_x, count_y):
    extent_x, wide_y, channels, lanes = cells.shape
    extent_y = wide_y - 2
    depth = lanes // 2
    out_channels = weights.shape[1]
    layers = depth // 2 // count_y
    mix = weights.transpose(1, 0, 2).reshape(out_channels, 27 * channels)
    return pl.pallas_call(
        functools.partial(three_kernel, layers),
        name="three",
        out_shape=(
            local((extent_x, extent_y // 2, out_channels, lanes)),
            local((count_x, count_y, extent_x // 2 * 8, extent_y // 2 * out_channels)),
        ),
        in_specs=[VMEM] * 5,
        out_specs=(VMEM, VMEM),
        scratch_shapes=[pltpu.VMEM((extent_x + 2, extent_y + 1, 3, channels, lanes), BF16)],
        cost_estimate=COST,
        compiler_params=pltpu.CompilerParams(vmem_limit_bytes=16 << 20),
    )(*map(near_memory, (cells, left, right, mix, bias_values)))


def four_kernel(count_y, tiles, weights, bias, columns, out, three_out, rolled, mix):
    _, parts, lanes = tiles.shape
    extent_x, extent_y, layers, out_channels = out.shape
    rows = count_y * 8
    inner_x = parts // 8
    half = lanes // 2
    upper = lax.broadcasted_iota(jnp.int32, (rows, lanes), 1) >= half
    short = count_y * layers
    for x in range(extent_x):
        start = x // inner_x * count_y
        at = x % inner_x * 8
        value = tiles[start : start + count_y, at : at + 8].reshape(rows, lanes).astype(F32)
        before = pltpu.roll(value, 8, 0)
        after = pltpu.roll(value, rows - 8, 0)
        around = pltpu.roll(jnp.where(upper, before, after), half, 1)
        whole = jnp.concatenate([value, around], axis=1)
        for e in range(3):
            turned = whole if e == 0 else pltpu.roll(whole, rows - e, 0)
            turned = turned.reshape(count_y, 8, 2 * lanes)[:, :layers].reshape(short, 2 * lanes)
            rolled[x + 1, :, e * 2 * lanes : (e + 1) * 2 * lanes] = turned.astype(BF16)
    rolled[0] = rolled[extent_x]
    rolled[extent_x + 1] = rolled[1]
    bands = ((1, 0), (2, 1), (0, None), (None, 2))
    for a in range(3):
        for e in range(3):
            for band, taps in enumerate(bands):
                row = ((3 * a + e) * 4 + band) * half
                for index, c in enumerate(taps):
                    lane = index * out_channels
                    if c is None:
                        tap = jnp.zeros((half, out_channels), BF16)
                    else:
                        tap = weights[9 * a + 3 * c + e]
                    mix[row : row + half, lane : lane + out_channels] = tap
    depth = three_out.shape[3]
    for x in range(columns.shape[0]):
        rows_of_y = [
            columns[x, pair][None, :, part * depth : (part + 1) * depth]
            for pair in range(columns.shape[1])
            for part in range(2)
        ]
        three_out[:, x] = jnp.swapaxes(jnp.concatenate(rows_of_y, axis=0), 0, 1)
    offset = jnp.concatenate([bias[...], bias[...]], axis=1)
    matrix = mix[...]
    group = min(extent_x, 4)
    for x in range(0, extent_x, group):
        stacked = jnp.concatenate(
            [rolled[x + a : x + a + group].reshape(group * short, 6 * lanes) for a in range(3)],
            axis=1,
        )
        result = jnp.dot(stacked, matrix, preferred_element_type=F32)
        result = leaky(result + offset).astype(BF16)
        for dx in range(group):
            for y in range(extent_y):
                row = dx * short + y // 2 * layers
                lane = y % 2 * out_channels
                out[x + dx, y] = result[row : row + layers, lane : lane + out_channels]


def four(tiles, weights, bias, columns, extents, count_y):
    extent_x, extent_y, layers = extents
    three_x, pairs, three_channels, lanes = columns.shape
    _, channels, out_channels = weights.shape
    return pl.pallas_call(
        functools.partial(four_kernel, count_y),
        name="four",
        out_shape=(
            jax.ShapeDtypeStruct((extent_x, extent_y, layers, out_channels), BF16),
            jax.ShapeDtypeStruct((three_channels, three_x, 2 * pairs, lanes // 2), BF16),
        ),
        in_specs=[VMEM] * 4,
        out_specs=(VMEM, VMEM),
        scratch_shapes=[
            pltpu.VMEM((extent_x + 2, count_y * layers, 6 * tiles.shape[2]), BF16),
            pltpu.VMEM((36 * channels, 2 * out_channels), BF16),
        ],
        cost_estimate=COST,
        compiler_params=pltpu.CompilerParams(vmem_limit_bytes=16 << 20),
    )(*map(near_memory, (tiles, weights, bias, columns)))


def shards(features, weight_two, bias_two, weight_three, bias_three, weight_four, bias_four):
    count_x, count_y = lax.axis_size("gx"), lax.axis_size("gy")
    width = 3
    channels, extent_x, extent_y, depth = features.shape
    even = lax.axis_index("gy") % 2 == 0
    flip = 1 - even.astype(jnp.int32)[None]
    cells, head, tail = split(flip, features, width)
    near_pairs, far_pairs = pairings("gy")
    far = lax.ppermute(head, "gy", far_pairs)
    near = lax.ppermute(tail, "gy", near_pairs)
    left, right = shift_exchange(
        jnp.concatenate([cells[0], near[0]], axis=0),
        jnp.concatenate([cells[-1], near[-1]], axis=0),
        "gx",
    )
    far_left, far_right = shift_exchange(far[0], far[-1], "gx")
    biases = [bias[None, :] for bias in (bias_two, bias_three, bias_four)]
    mix, bias, bias_three, bias_four = kernel_call(
        mix_kernel,
        flip,
        [weight_two, *biases],
        [local((4 * channels, 48 * channels))] + [pltpu.VMEM(row.shape, F32) for row in biases],
        [],
    )
    rest = extent_y // 2
    deep = extent_y + width - 1

    def main_call(body, name, operands, blocks):
        read = 2 * blocks + 2 if name == "center_two" else 8
        return kernel_call(
            body,
            flip,
            [cells, near, *operands, mix, bias],
            [
                (2 * blocks, extent_y - 2, channels, depth),
                (blocks, rest, channels, depth),
                (3, read, width, channels, depth),
            ],
            [(3, read, deep, channels, depth)],
        )

    center, center_pooled, center_edge = main_call(
        center_two_kernel, "center_two", [], extent_x // 2 - 2
    )
    sides, sides_pooled, sides_edge = main_call(
        sides_two_kernel, "sides_two", [left, right], 2
    )
    rim = (3, extent_x + 2, width, channels, depth)
    middle, middle_pooled = kernel_call(
        middle_two_kernel,
        flip,
        [far, center_edge, mix, bias],
        [(extent_x - 4, 2, channels, depth), (extent_x // 2 - 2, 2, channels, depth)],
        [rim],
    )
    far_out, pooled, low, high = kernel_call(
        corner_two_kernel,
        flip,
        [
            far, far_left, far_right, sides_edge, mix, bias,
            middle, middle_pooled, center_pooled, sides_pooled,
        ],
        [
            (extent_x, 2, channels, depth),
            (extent_x // 2, rest + 2, channels, depth),
            (rest // 2 + 1, channels, depth),
            (rest // 2 + 1, channels, depth),
        ],
        [rim, (extent_x // 2, 2, channels, depth)],
    )
    level_two = store_two(flip, far_out, center, sides)

    left, right = shift_exchange(low, high, "gx")
    columns, windows = three(
        pooled, left, right, weight_three, bias_three, count_x, count_y
    )
    slots = count_x * count_y
    tiles = lax.all_to_all(
        windows.reshape((slots,) + windows.shape[2:]), ("gx", "gy"), 0, 0, tiled=True
    )
    extents = (count_x * extent_x // 4, count_y * extent_y // 4, depth // 4 // count_y)
    bottleneck, level_three = four(
        tiles, weight_four.transpose(0, 2, 1), bias_four, columns, extents, count_y
    )
    return level_two, level_three, bottleneck.transpose(3, 0, 1, 2)


def solution(mesh):
    return jax.shard_map(
        shards,
        mesh=mesh,
        in_specs=(P(None, "gx", "gy", None), P(), P(), P(), P(), P(), P()),
        out_specs=(
            P(None, "gx", "gy", None),
            P(None, "gx", "gy", None),
            P(None, None, None, "gy"),
        ),
        check_vma=False,
    )
```

```python
import functools

import jax
import jax.numpy as jnp
from jax import lax
from jax.experimental import pallas as pl
from jax.experimental.pallas import tpu as pltpu
from jax.sharding import PartitionSpec as P


VMEM = pl.BlockSpec(memory_space=pltpu.VMEM)
BF16 = jnp.bfloat16
F32 = jnp.float32
SCALAR = pl.BlockSpec(memory_space=pltpu.SMEM)
COST = pl.CostEstimate(flops=1 << 30, transcendentals=0, bytes_accessed=1 << 20)


def leaky(t):
    return jnp.where(t >= 0, t, 0.1 * t)


def near_memory(value):
    return pltpu.with_memory_space_constraint(value, pltpu.VMEM)


def local(shape):
    return pltpu.VMEM(shape, BF16)


def column(bias):
    count = bias.shape[1]
    return jnp.broadcast_to(bias[...], (count, count)).T[:, :1]


def shift_exchange(low, high, axis):
    count = lax.axis_size(axis)
    below = lax.ppermute(high, axis, [(i, (i + 1) % count) for i in range(count)])
    above = lax.ppermute(low, axis, [((i + 1) % count, i) for i in range(count)])
    return below, above


def pairings(axis):
    count = lax.axis_size(axis)
    near = [(i, i + 1 if i % 2 == 0 else i - 1) for i in range(count)]
    far = [(i, (i - 1) % count if i % 2 == 0 else (i + 1) % count) for i in range(count)]
    return near, far


def mix_two(mix, bias, pool, stacked, channels, depth):
    result = jnp.dot(mix, stacked, preferred_element_type=F32)
    result = leaky(result + bias).astype(BF16)
    answers = []
    for half in range(result.shape[1] // depth):
        block = result[:, half * depth : (half + 1) * depth]
        sums = jnp.dot(block, pool, preferred_element_type=F32)
        mean = sums[:channels]
        for part in range(1, 4):
            mean = mean + sums[part * channels : (part + 1) * channels]
        answers.append((block, mean.astype(BF16)))
    return answers


def pool_two(depth):
    source = lax.broadcasted_iota(jnp.int32, (depth, depth), 0) // 2
    target = lax.broadcasted_iota(jnp.int32, (depth, depth), 1) % (depth // 2)
    return jnp.where(source == target, 0.125, 0.0).astype(BF16)


def shifts(value):
    depth = value.shape[1]
    return pltpu.roll(value, 1, 1), value, pltpu.roll(value, depth - 1, 1)


def split_kernel(flip, features, cells, head, tail, parts, arrived):
    _, extent_y = cells.shape[:2]
    count, _, step = parts.shape[:3]
    turn = flip[0]
    copies = [
        pltpu.make_async_copy(
            features.at[:, pl.ds(part * step, step)], parts.at[part], arrived.at[part]
        )
        for part in range(count)
    ]
    for copy in copies:
        copy.start()
    for part in range(count):
        copies[part].wait()
        for index in range(step):
            x = part * step + index
            cells[x] = jnp.swapaxes(parts[part, :, index], 0, 1)
            for row in range(head.shape[1]):
                head[x, row] = cells[x, mirrored(row, extent_y, turn)]
                tail[x, row] = cells[x, mirrored(extent_y - 1 - row, extent_y, turn)]


def split(flip, features, width):
    channels, extent_x, extent_y, depth = features.shape
    step = 2
    count = extent_x // step
    return pl.pallas_call(
        split_kernel,
        name="split",
        out_shape=(
            local((extent_x, extent_y, channels, depth)),
            local((extent_x, width, channels, depth)),
            local((extent_x, width, channels, depth)),
        ),
        in_specs=[SCALAR, pl.BlockSpec(memory_space=pl.ANY)],
        out_specs=(VMEM,) * 3,
        scratch_shapes=[
            pltpu.VMEM((count, channels, step, extent_y, depth), BF16),
            pltpu.SemaphoreType.DMA((count,)),
        ],
        cost_estimate=COST,
        compiler_params=pltpu.CompilerParams(vmem_limit_bytes=16 << 20),
    )(flip, pltpu.with_memory_space_constraint(features, pltpu.HBM))


def mix_kernel(flip, weights, *refs):
    count = len(refs) // 2
    mix = refs[count]
    for source, target in zip(refs[:count], refs[count + 1 :]):
        target[...] = source[...]
    channels = weights.shape[1]
    blank = jnp.zeros((channels, channels), BF16)
    empty = jnp.zeros((channels, 4 * channels), BF16)
    turn = flip[0]
    for e in range(3):
        for a in range(3):
            taps = [weights[9 * a + e + 3 * (c + turn * (2 - 2 * c))] for c in range(3)]
            for dy in range(2):
                tile = jnp.concatenate([blank] * dy + taps + [blank] * (1 - dy), axis=1)
                for dx in range(2):
                    row = (2 * dx + dy) * channels
                    at = (4 * e + a + dx) * 4 * channels
                    mix[row : row + channels, at : at + 4 * channels] = tile
        for dy in range(2):
            for dx in range(2):
                row = (2 * dx + dy) * channels
                at = (4 * e + 3 * (1 - dx)) * 4 * channels
                mix[row : row + channels, at : at + 4 * channels] = empty


def store_block(block, target, x, y, turn, channels):
    for part in range(4):
        dx, dy = part // 2, part % 2
        target[x + dx, y + dy + turn * (1 - 2 * dy)] = block[
            part * channels : (part + 1) * channels
        ]


def frames(blocks):
    return sorted({at for start in blocks for at in range(start, start + 4)})


def main_two(blocks, fetch, extent_y, mix, bias, turn, out, pooled, edge, rolled):
    width, channels, depth = edge.shape[2:]
    columns = frames(blocks)
    for slot, x in enumerate(columns):
        for y in range(extent_y + width):
            for e, turned in enumerate(shifts(fetch(x, y))):
                if y < width:
                    edge[e, slot, y] = turned
                if y:
                    rolled[e, slot, y - 1] = turned
    offset = jnp.concatenate([column(bias)] * 4, axis=0)
    pool = pool_two(depth)
    matrix = mix[...]
    for index, x in enumerate(blocks):
        slot = columns.index(x)
        rows = list(range(2, extent_y + 1, 2))
        stacked = jnp.concatenate(
            [
                rolled[:, slot : slot + 4, y - 2 : y + 2].reshape(48 * channels, depth)
                for y in rows
            ],
            axis=1,
        )
        answers = mix_two(matrix, offset, pool, stacked, channels, depth)
        for y, (block, mean) in zip(rows, answers):
            if y < extent_y:
                at = y - 2 + turn * (extent_y - 2 * y)
                store_block(block, out, 2 * index, at, turn, channels)
            pooled[index, y // 2 - 1 + turn * (extent_y // 2 + 1 - y)] = mean


def mirrored(y, extent_y, turn):
    return y + turn * (extent_y - 1 - 2 * y) if y < extent_y else y


def center_two_kernel(flip, cells, near, mix, bias, out, pooled, edge, rolled):
    extent_x, extent_y = cells.shape[:2]

    def fetch(x, y):
        if y < extent_y:
            return cells[x - 1, mirrored(y, extent_y, flip[0])]
        return near[x - 1, y - extent_y]

    blocks = list(range(2, extent_x - 2, 2))
    main_two(blocks, fetch, extent_y, mix, bias, flip[0], out, pooled, edge, rolled)


def sides_two_kernel(flip, cells, near, left, right, mix, bias, out, pooled, edge, rolled):
    extent_x, extent_y = cells.shape[:2]

    def fetch(x, y):
        at = mirrored(y, extent_y, flip[0])
        if x == 0:
            return left[at]
        if x == extent_x + 1:
            return right[at]
        if y < extent_y:
            return cells[x - 1, at]
        return near[x - 1, y - extent_y]

    blocks = [0, extent_x - 2]
    main_two(blocks, fetch, extent_y, mix, bias, flip[0], out, pooled, edge, rolled)


def far_two(blocks, fetch, edge, mix, bias, turn, out, pooled, shift, rim):
    _, _, width, channels, depth = edge.shape
    columns = frames(blocks)
    for x in columns:
        for row in range(width):
            for e, turned in enumerate(shifts(fetch(x, row))):
                rim[e, x, width - 1 - row] = turned
    offset = jnp.concatenate([column(bias)] * 4, axis=0)
    pool = pool_two(depth)
    starts = [(x, first) for x in blocks for first in (0, 2)]
    stacked = jnp.concatenate(
        [
            jnp.concatenate(
                [
                    piece.reshape(-1, depth)
                    for e in range(3)
                    for at in range(x, x + 4)
                    for piece in (
                        rim[e, at, first:],
                        edge[e, columns.index(at), : first + 4 - width],
                    )
                ],
                axis=0,
            )
            for x, first in starts
        ],
        axis=1,
    )
    answers = mix_two(mix[...], offset, pool, stacked, channels, depth)
    for (x, first), (block, mean) in zip(starts, answers):
        if first:
            store_block(block, out, x - shift, 0, turn, channels)
        own = first // 2
        pooled[(x - shift) // 2, own + turn * (1 - 2 * own)] = mean


def middle_two_kernel(flip, far, edge, mix, bias, out, pooled, rim):
    extent_x = far.shape[0]
    far_two(
        list(range(2, extent_x - 2, 2)),
        lambda x, row: far[x - 1, row],
        edge,
        mix,
        bias,
        flip[0],
        out,
        pooled,
        2,
        rim,
    )


def corner_two_kernel(
    flip, far, left, right, edge, mix, bias, middle, middle_pooled, center_pooled, sides_pooled,
    out, pooled, low, high, rim, means,
):
    extent_x = far.shape[0]
    turn = flip[0]

    def fetch(x, row):
        if x == 0:
            return left[row]
        if x == extent_x + 1:
            return right[row]
        return far[x - 1, row]

    far_two([0, extent_x - 2], fetch, edge, mix, bias, turn, out, means, 0, rim)
    out[2 : extent_x - 2] = middle[...]
    means[1 : extent_x // 2 - 1] = middle_pooled[...]
    rest = center_pooled.shape[1]
    pooled[:, pl.ds(turn * rest, 2)] = means[...]
    main = pl.ds(2 - 2 * turn, rest)
    last = extent_x // 2 - 1
    pooled[0:1, main] = sides_pooled[0:1]
    pooled[1:last, main] = center_pooled[...]
    pooled[last : last + 1, main] = sides_pooled[1:2]
    channels, depth = low.shape[1:]
    first = lax.broadcasted_iota(jnp.int32, (channels, depth), 1) < depth // 2
    for target, x in ((low, 0), (high, extent_x // 2 - 1)):
        for pair in range(target.shape[0]):
            target[pair] = jnp.where(first, pooled[x, 2 * pair], pooled[x, 2 * pair + 1])


def kernel_call(body, flip, operands, results, scratch):
    return pl.pallas_call(
        body,
        out_shape=tuple(
            local(result) if isinstance(result, tuple) else result for result in results
        ),
        in_specs=[SCALAR] + [VMEM] * len(operands),
        out_specs=(VMEM,) * len(results),
        scratch_shapes=[pltpu.VMEM(shape, BF16) for shape in scratch],
        cost_estimate=COST,
        compiler_params=pltpu.CompilerParams(vmem_limit_bytes=16 << 20),
    )(flip, *map(near_memory, operands))


def store_two_kernel(flip, far, center, sides, out, rows):
    extent_x = far.shape[0]
    extent_y = out.shape[2]
    turn = flip[0]
    for x in range(extent_x):
        if 2 <= x < extent_x - 2:
            main = center[x - 2]
        else:
            main = sides[x if x < 2 else x - extent_x + 4]
        rows[x, pl.ds(turn * (extent_y - 2), 2)] = far[x]
        rows[x, pl.ds(2 - 2 * turn, extent_y - 2)] = main
        out[:, x] = jnp.swapaxes(rows[x], 0, 1)


def store_two(flip, far, center, sides):
    extent_x, _, channels, depth = far.shape
    extent_y = center.shape[1] + 2
    return pl.pallas_call(
        store_two_kernel,
        name="store_two",
        out_shape=jax.ShapeDtypeStruct((channels, extent_x, extent_y, depth), BF16),
        in_specs=[SCALAR] + [VMEM] * 3,
        out_specs=VMEM,
        scratch_shapes=[pltpu.VMEM((extent_x, extent_y, channels, depth), BF16)],
        cost_estimate=COST,
        compiler_params=pltpu.CompilerParams(vmem_limit_bytes=16 << 20),
    )(flip, *map(near_memory, (far, center, sides)))


def pair_columns(turned, target, at):
    channels, lanes = turned[0][0].shape
    first = lax.broadcasted_iota(jnp.int32, (channels, lanes), 1) < lanes // 2
    for y in range(len(turned) - 1):
        for e in range(3):
            target[at, y, e] = jnp.where(first, turned[y][e], turned[y + 1][e])


def mix_three(matrix, offset, columns, pairs):
    pieces = []
    for frame, py in pairs:
        taps = [
            source[at, 2 * py + c].reshape(-1, source.shape[4])
            for source, at in frame
            for c in range(3)
        ]
        pieces.append(jnp.concatenate(taps, axis=0))
    stacked = jnp.concatenate(pieces, axis=1)
    result = leaky(jnp.dot(matrix, stacked, preferred_element_type=F32) + offset).astype(BF16)
    return [result[:, at * columns : (at + 1) * columns] for at in range(len(pairs))]


def own_three_kernel(cells, mix, bias, inside, paired):
    extent_x, wide_y, _, lanes = cells.shape
    for x in range(extent_x):
        pair_columns([shifts(cells[x, y]) for y in range(wide_y)], paired, x)
    offset = column(bias)
    matrix = mix[...]
    for py in range((wide_y - 2) // 2):
        places = range(1, extent_x - 1)
        pairs = [([(paired, x + a) for a in (-1, 0, 1)], py) for x in places]
        for x, part in zip(places, mix_three(matrix, offset, lanes, pairs)):
            inside[x - 1, py] = part


def three_kernel(layers, paired, inside, left, right, mix, bias, out, windows, outer):
    extent_x, wide_y, _, channels, lanes = paired.shape
    extent_y = wide_y - 1
    depth = lanes // 2
    senders, slots = windows.shape[:2]
    first = lax.broadcasted_iota(jnp.int32, (channels, lanes), 1) < depth
    for side, source in enumerate((left, right)):
        turned = []
        for y in range(extent_y + 2):
            both = source[y // 2]
            both = jnp.where(first == (y % 2 == 0), both, pltpu.roll(both, depth, 1))
            turned.append(shifts(both))
        pair_columns(turned, outer, side)
    offset = column(bias)
    rows = lax.broadcasted_iota(jnp.int32, (slots * 8, 2 * lanes), 0)
    layer = rows % 8
    wanted = (layers * (rows // 8) + layer + depth // 2 - 1) % (depth // 2)
    source = lax.broadcasted_iota(jnp.int32, (slots * 8, 2 * lanes), 1) % depth // 2
    pool = jnp.where((source == wanted) & (layer < layers + 2), 0.125, 0.0).astype(BF16)
    last = extent_x - 1
    ends = (
        [(outer, 0), (paired, 0), (paired, 1)],
        [(paired, last - 1), (paired, last), (outer, 1)],
    )
    pairs = [(frame, py) for frame in ends for py in range(extent_y // 2)]
    parts = mix_three(mix[...], offset, lanes, pairs)
    for at, part in enumerate(parts):
        out[last * (at // (extent_y // 2)), at % (extent_y // 2)] = part
    out[1:last] = inside[...]
    for px in range(extent_x // 2):
        results = [
            jnp.concatenate([out[2 * px, py], out[2 * px + 1, py]], axis=1)
            for py in range(extent_y // 2)
        ]
        means = lax.dot_general(
            pool,
            jnp.concatenate(results, axis=0),
            (((1,), (1,)), ((), ())),
            preferred_element_type=F32,
        ).astype(BF16)
        for slot in range(slots):
            for sender in range(senders):
                windows[sender, slot, 8 * px : 8 * px + 8] = means[8 * slot : 8 * slot + 8]


def own_three(cells, mix, bias):
    extent_x, wide_y, channels, lanes = cells.shape
    return pl.pallas_call(
        own_three_kernel,
        name="own_three",
        out_shape=(
            local((extent_x - 2, (wide_y - 2) // 2, mix.shape[0], lanes)),
            local((extent_x, wide_y - 1, 3, channels, lanes)),
        ),
        in_specs=[VMEM] * 3,
        out_specs=(VMEM, VMEM),
        cost_estimate=COST,
        compiler_params=pltpu.CompilerParams(vmem_limit_bytes=16 << 20),
    )(*map(near_memory, (cells, mix, bias)))


def three(paired, inside, left, right, mix, bias, count_x, count_y):
    extent_x, wide_y, _, channels, lanes = paired.shape
    extent_y = wide_y - 1
    out_channels = mix.shape[0]
    layers = lanes // 4 // count_y
    return pl.pallas_call(
        functools.partial(three_kernel, layers),
        name="three",
        out_shape=(
            local((extent_x, extent_y // 2, out_channels, lanes)),
            local((count_x, count_y, extent_x // 2 * 8, extent_y // 2 * out_channels)),
        ),
        in_specs=[VMEM] * 6,
        out_specs=(VMEM, VMEM),
        scratch_shapes=[pltpu.VMEM((2, wide_y, 3, channels, lanes), BF16)],
        cost_estimate=COST,
        compiler_params=pltpu.CompilerParams(vmem_limit_bytes=16 << 20),
    )(*map(near_memory, (paired, inside, left, right, mix, bias)))


def four_kernel(count_y, tiles, weights, bias, columns, out, three_out, rolled, mix):
    _, parts, lanes = tiles.shape
    extent_x, extent_y, layers, out_channels = out.shape
    rows = count_y * 8
    inner_x = parts // 8
    half = lanes // 2
    upper = lax.broadcasted_iota(jnp.int32, (rows, lanes), 1) >= half
    short = count_y * layers
    for x in range(extent_x):
        start = x // inner_x * count_y
        at = x % inner_x * 8
        value = tiles[start : start + count_y, at : at + 8].reshape(rows, lanes).astype(F32)
        before = pltpu.roll(value, 8, 0)
        after = pltpu.roll(value, rows - 8, 0)
        around = pltpu.roll(jnp.where(upper, before, after), half, 1)
        whole = jnp.concatenate([value, around], axis=1)
        for e in range(3):
            turned = whole if e == 0 else pltpu.roll(whole, rows - e, 0)
            turned = turned.reshape(count_y, 8, 2 * lanes)[:, :layers].reshape(short, 2 * lanes)
            rolled[x + 1, :, e * 2 * lanes : (e + 1) * 2 * lanes] = turned.astype(BF16)
    rolled[0] = rolled[extent_x]
    rolled[extent_x + 1] = rolled[1]
    bands = ((1, 0), (2, 1), (0, None), (None, 2))
    for a in range(3):
        for e in range(3):
            for band, taps in enumerate(bands):
                row = ((3 * a + e) * 4 + band) * half
                for index, c in enumerate(taps):
                    lane = index * out_channels
                    if c is None:
                        tap = jnp.zeros((half, out_channels), BF16)
                    else:
                        tap = weights[9 * a + 3 * c + e]
                    mix[row : row + half, lane : lane + out_channels] = tap
    depth = three_out.shape[3]
    for x in range(columns.shape[0]):
        rows_of_y = [
            columns[x, pair][None, :, part * depth : (part + 1) * depth]
            for pair in range(columns.shape[1])
            for part in range(2)
        ]
        three_out[:, x] = jnp.swapaxes(jnp.concatenate(rows_of_y, axis=0), 0, 1)
    offset = jnp.concatenate([bias[...], bias[...]], axis=1)
    matrix = mix[...]
    group = min(extent_x, 4)
    for x in range(0, extent_x, group):
        stacked = jnp.concatenate(
            [rolled[x + a : x + a + group].reshape(group * short, 6 * lanes) for a in range(3)],
            axis=1,
        )
        result = jnp.dot(stacked, matrix, preferred_element_type=F32)
        result = leaky(result + offset).astype(BF16)
        for dx in range(group):
            for y in range(extent_y):
                row = dx * short + y // 2 * layers
                lane = y % 2 * out_channels
                out[x + dx, y] = result[row : row + layers, lane : lane + out_channels]


def four(tiles, weights, bias, columns, extents, count_y):
    extent_x, extent_y, layers = extents
    three_x, pairs, three_channels, lanes = columns.shape
    _, channels, out_channels = weights.shape
    return pl.pallas_call(
        functools.partial(four_kernel, count_y),
        name="four",
        out_shape=(
            jax.ShapeDtypeStruct((extent_x, extent_y, layers, out_channels), BF16),
            jax.ShapeDtypeStruct((three_channels, three_x, 2 * pairs, lanes // 2), BF16),
        ),
        in_specs=[VMEM] * 4,
        out_specs=(VMEM, VMEM),
        scratch_shapes=[
            pltpu.VMEM((extent_x + 2, count_y * layers, 6 * tiles.shape[2]), BF16),
            pltpu.VMEM((36 * channels, 2 * out_channels), BF16),
        ],
        cost_estimate=COST,
        compiler_params=pltpu.CompilerParams(vmem_limit_bytes=16 << 20),
    )(*map(near_memory, (tiles, weights, bias, columns)))


def shards(features, weight_two, bias_two, weight_three, bias_three, weight_four, bias_four):
    count_x, count_y = lax.axis_size("gx"), lax.axis_size("gy")
    width = 3
    channels, extent_x, extent_y, depth = features.shape
    even = lax.axis_index("gy") % 2 == 0
    flip = 1 - even.astype(jnp.int32)[None]
    cells, head, tail = split(flip, features, width)
    near_pairs, far_pairs = pairings("gy")
    far = lax.ppermute(head, "gy", far_pairs)
    near = lax.ppermute(tail, "gy", near_pairs)
    left, right = shift_exchange(
        jnp.concatenate([cells[0], near[0]], axis=0),
        jnp.concatenate([cells[-1], near[-1]], axis=0),
        "gx",
    )
    far_left, far_right = shift_exchange(far[0], far[-1], "gx")
    biases = [bias[None, :] for bias in (bias_two, bias_three, bias_four)]
    mix, bias, bias_three, bias_four = kernel_call(
        mix_kernel,
        flip,
        [weight_two, *biases],
        [local((4 * channels, 48 * channels))] + [pltpu.VMEM(row.shape, F32) for row in biases],
        [],
    )
    rest = extent_y // 2
    deep = extent_y + width - 1

    def main_call(body, name, operands, blocks):
        read = 2 * blocks + 2 if name == "center_two" else 8
        return kernel_call(
            body,
            flip,
            [cells, near, *operands, mix, bias],
            [
                (2 * blocks, extent_y - 2, channels, depth),
                (blocks, rest, channels, depth),
                (3, read, width, channels, depth),
            ],
            [(3, read, deep, channels, depth)],
        )

    center, center_pooled, center_edge = main_call(
        center_two_kernel, "center_two", [], extent_x // 2 - 2
    )
    sides, sides_pooled, sides_edge = main_call(
        sides_two_kernel, "sides_two", [left, right], 2
    )
    rim = (3, extent_x + 2, width, channels, depth)
    middle, middle_pooled = kernel_call(
        middle_two_kernel,
        flip,
        [far, center_edge, mix, bias],
        [(extent_x - 4, 2, channels, depth), (extent_x // 2 - 2, 2, channels, depth)],
        [rim],
    )
    far_out, pooled, low, high = kernel_call(
        corner_two_kernel,
        flip,
        [
            far, far_left, far_right, sides_edge, mix, bias,
            middle, middle_pooled, center_pooled, sides_pooled,
        ],
        [
            (extent_x, 2, channels, depth),
            (extent_x // 2, rest + 2, channels, depth),
            (rest // 2 + 1, channels, depth),
            (rest // 2 + 1, channels, depth),
        ],
        [rim, (extent_x // 2, 2, channels, depth)],
    )
    level_two = store_two(flip, far_out, center, sides)

    left, right = shift_exchange(low, high, "gx")
    three_mix = weight_three.transpose(1, 0, 2).reshape(weight_three.shape[1], -1)
    inside, paired = own_three(pooled, three_mix, bias_three)
    columns, windows = three(
        paired, inside, left, right, three_mix, bias_three, count_x, count_y
    )
    slots = count_x * count_y
    tiles = lax.all_to_all(
        windows.reshape((slots,) + windows.shape[2:]), ("gx", "gy"), 0, 0, tiled=True
    )
    extents = (count_x * extent_x // 4, count_y * extent_y // 4, depth // 4 // count_y)
    bottleneck, level_three = four(
        tiles, weight_four.transpose(0, 2, 1), bias_four, columns, extents, count_y
    )
    return level_two, level_three, bottleneck.transpose(3, 0, 1, 2)


def solution(mesh):
    return jax.shard_map(
        shards,
        mesh=mesh,
        in_specs=(P(None, "gx", "gy", None), P(), P(), P(), P(), P(), P()),
        out_specs=(
            P(None, "gx", "gy", None),
            P(None, "gx", "gy", None),
            P(None, None, None, "gy"),
        ),
        check_vma=False,
    )
```
